8 devices in a mesh: data: 2 (over z, y), seq: 4 (over x, core).
Axes of the slice: x: 2, y: 2, z: 1, core: 2. Of those that a mesh axis runs over, the one named last changes fastest.
Arguments:
- tokens: bfloat16 [8, 1024, 384], P('data', 'seq'), parts along dimension 0
- lengths: int32 [8], P('data'), parts along dimension 0
- slot_param: bfloat16 [384, 4096], replicated
- logit_scale: float32 [], replicated
- w_in: bfloat16 [256, 384, 1536], P('seq')
- w_out: bfloat16 [256, 1536, 384], P('seq')
Outputs:
- output: bfloat16 [8, 1024, 384], P('data', 'seq'), parts along dimension 0
There are 2 independent parts. The reference program is written for one: setup_inputs(seed, part) draws one part's arguments, and reference() takes and returns one part's arrays. A program takes and returns all parts, laid end to end along the dimension named above; an argument that names none is the same for every part.
All inputs are finite; a program needn't handle non-finite values.
Results may differ from the reference program's by a relative error of at most 0.0138026.
Values are sent between devices in bfloat16 or wider.
A program may use at most 1 GiB of HBM per device.

```python
import jax
import jax.numpy as jnp
from jax import lax

BATCH = 4
TOKENS = 1024
D_MODEL = 384
FF_DIM = 1536
EXPERTS = 256
SLOTS = 16
LATENT = 16

N_SLOTS = EXPERTS * SLOTS
EPSILON = 1e-6
NEG_FILL = -1e30


def setup_inputs(seed: int = 0, part: int = 0) -> dict:
    shared = jax.random.split(jax.random.key(seed), 6)
    own = jax.random.split(jax.random.fold_in(jax.random.key(seed + 1), part), 3)
    basis = jax.random.normal(shared[0], (LATENT, D_MODEL), jnp.float32)
    phi_code = jax.random.normal(shared[1], (LATENT, N_SLOTS), jnp.float32)
    slot_param = jnp.dot(basis.T, phi_code) / LATENT ** 0.5 + 0.5 * jax.random.normal(shared[2], (D_MODEL, N_SLOTS), jnp.float32)
    logit_scale = 6.0 + 4.0 * jax.random.uniform(shared[3], (), jnp.float32)
    w_in = 2.0 * D_MODEL ** -0.5 * jax.random.normal(shared[4], (EXPERTS, D_MODEL, FF_DIM), jnp.float32)
    w_out = 2.0 * FF_DIM ** -0.5 * jax.random.normal(shared[5], (EXPERTS, FF_DIM, D_MODEL), jnp.float32)
    tok_code = jax.random.normal(own[0], (BATCH, TOKENS, LATENT), jnp.float32)
    tokens = jnp.einsum("btl,ld->btd", tok_code, basis) / LATENT ** 0.5 + 0.5 * jax.random.normal(own[1], (BATCH, TOKENS, D_MODEL), jnp.float32)
    drawn = jax.random.randint(own[2], (BATCH,), 1, TOKENS + 1, jnp.int32)
    lengths = jnp.where(jnp.arange(BATCH) == 0, TOKENS, drawn).astype(jnp.int32)
    return {"tokens": tokens.astype(jnp.bfloat16), "lengths": lengths, "slot_param": slot_param.astype(jnp.bfloat16), "logit_scale": logit_scale, "w_in": w_in.astype(jnp.bfloat16), "w_out": w_out.astype(jnp.bfloat16)}


def l2_normed(values, axis_dim):
    v32 = values.astype(jnp.float32)
    return (v32 * lax.rsqrt(jnp.sum(v32 * v32, axis=axis_dim, keepdims=True) + EPSILON)).astype(jnp.bfloat16)


def reference(tokens, lengths, slot_param, logit_scale, w_in, w_out):
    phi_norm = l2_normed(slot_param, 0).astype(jnp.float32)
    positions = jnp.arange(TOKENS, dtype=jnp.int32)

    def row_logits(tok_row):
        tok_norm = l2_normed(tok_row, 1).astype(jnp.float32)
        return logit_scale * jnp.dot(tok_norm, phi_norm, preferred_element_type=jnp.float32)

    def dispatch_row(row_args):
        tok_row, len_row = row_args
        logits = row_logits(tok_row)
        masked = jnp.where((positions < len_row)[:, None], logits, NEG_FILL)
        disp_w = jnp.exp(masked - jnp.max(masked, axis=0, keepdims=True))
        col_sum = jnp.sum(disp_w, axis=0)
        slot_sum = jnp.dot(disp_w.astype(jnp.bfloat16).astype(jnp.float32).T, tok_row.astype(jnp.float32), preferred_element_type=jnp.float32)
        return (slot_sum / col_sum[:, None]).astype(jnp.bfloat16)

    slot_in = lax.map(dispatch_row, (tokens, lengths))
    slot_grp = jnp.transpose(slot_in.reshape(BATCH, EXPERTS, SLOTS, D_MODEL), (1, 0, 2, 3))

    def expert_ffn(exp_args):
        slot_exp, win_exp, wout_exp = exp_args
        hidden = jnp.einsum("bsd,df->bsf", slot_exp.astype(jnp.float32), win_exp.astype(jnp.float32))
        hidden = jax.nn.gelu(hidden).astype(jnp.bfloat16)
        return jnp.einsum("bsf,fd->bsd", hidden.astype(jnp.float32), wout_exp.astype(jnp.float32)).astype(jnp.bfloat16)

    slot_out = lax.map(expert_ffn, (slot_grp, w_in, w_out))
    slot_out = jnp.transpose(slot_out, (1, 0, 2, 3)).reshape(BATCH, N_SLOTS, D_MODEL)

    def combine_row(row_args):
        tok_row, len_row, out_row = row_args
        logits = row_logits(tok_row)
        comb_w = jnp.exp(logits - jnp.max(logits, axis=1, keepdims=True))
        row_sum = jnp.sum(comb_w, axis=1, keepdims=True)
        tok_mixed = jnp.dot(comb_w.astype(jnp.bfloat16).astype(jnp.float32), out_row.astype(jnp.float32), preferred_element_type=jnp.float32) / row_sum
        return jnp.where((positions < len_row)[:, None], tok_mixed, 0.0).astype(jnp.bfloat16)

    return lax.map(combine_row, (tokens, lengths, slot_out))
```

```python
import functools
import math

import jax
import jax.numpy as jnp
from jax import lax
from jax.experimental import pallas as pl
from jax.experimental.pallas import tpu as pltpu
from jax.sharding import PartitionSpec as P

EPSILON = 1e-6
NEG_FILL = -1e30
LOG2E = 1.0 / math.log(2.0)
F32 = jnp.float32
BF16 = jnp.bfloat16
RING = 7


def unit_rows(v32):
    return (v32 * lax.rsqrt(jnp.sum(v32 * v32, axis=1, keepdims=True) + EPSILON)).astype(BF16)


def gelu_tanh(h):
    inner = h * (math.sqrt(2.0 / math.pi) + (math.sqrt(2.0 / math.pi) * 0.044715) * (h * h))
    half = 0.5 * h
    return half + half * jnp.tanh(inner)


def row_of(col, rows):
    return jnp.broadcast_to(col, (rows, 128)).T[0:1, :]


def layer_kernel(
    scale_ref, len_ref, x_ref, phi_hbm, w1_hbm, w2_hbm, out_ref,
    xg, rm, qrow, pnt, ct, xs, d2r, hr, f1r, f2r, w1b, w2b,
    phi_sem, w1_sem, w2_sem,
    sx_sem, sy_sem, sp_sem, sf_sem, r0_sem, r1_sem,
    rms_sem, rm0_sem, rm1_sem,
    d2s_sem, d2r_sem, hs_sem, hr_sem, f1s_sem, f1r_sem, f2s_sem, f2r_sem,
):
    nb, tok, dm = x_ref.shape
    slots = pnt.shape[0]
    n_slots = phi_hbm.shape[1]
    n_exp = slots // 16
    d = lax.axis_index("data")
    s = lax.axis_index("seq")
    xc, core = s // 2, s % 2
    to_p = {"data": d, "seq": 2 * xc + (1 - core)}
    to_x = {"data": d, "seq": 2 * (1 - xc) + core}
    to_y = {"data": 1 - d, "seq": s}

    def remote(src, dst, send, recv, dev):
        return pltpu.make_async_remote_copy(src_ref=src, dst_ref=dst, send_sem=send, recv_sem=recv, device_id=dev, device_id_type=pl.DeviceIdType.MESH)

    def weight_copies(e, slot):
        return (
            pltpu.make_async_copy(w1_hbm.at[n_exp * d + e], w1b.at[slot], w1_sem.at[slot]),
            pltpu.make_async_copy(w2_hbm.at[n_exp * d + e], w2b.at[slot], w2_sem.at[slot]),
        )

    barrier = pltpu.get_barrier_semaphore()
    for dev in (to_p, to_x, to_y):
        pl.semaphore_signal(barrier, inc=1, device_id=dev, device_id_type=pl.DeviceIdType.MESH)

    def send_x(b):
        return remote(x_ref.at[b], xg.at[1, b, 0], sx_sem.at[b], r0_sem.at[4 + b], to_x)

    def send_y(b):
        return remote(x_ref.at[b], xg.at[2, b, 0], sy_sem.at[b], r0_sem.at[8 + b], to_y)

    def send_p(b):
        return remote(x_ref.at[b], xg.at[0, b, 1], sp_sem.at[b], r1_sem.at[b], to_p)

    def fwd_p(r, b):
        return remote(xg.at[r, b, 0], xg.at[r, b, 1], sp_sem.at[4 * r + b], r1_sem.at[4 * r + b], to_p)

    def fwd_y(b):
        return remote(xg.at[1, b, 0], xg.at[3, b, 0], sf_sem.at[b], r0_sem.at[12 + b], to_y)

    def fwd_x(b):
        return remote(xg.at[2, b, 0], xg.at[3, b, 0], sf_sem.at[b], r0_sem.at[12 + b], to_x)

    rm_x = remote(rm.at[0, 0], rm.at[1, 0], rms_sem.at[0], rm0_sem.at[1], to_x)
    rm_y = remote(rm.at[0, 0], rm.at[2, 0], rms_sem.at[1], rm0_sem.at[2], to_y)
    rm_f = remote(rm.at[1, 0], rm.at[3, 0], rms_sem.at[2], rm0_sem.at[3], to_y)
    rm_p = [remote(rm.at[r, 0], rm.at[r, 1], rms_sem.at[3 + r], rm1_sem.at[r], to_p) for r in range(4)]

    def phase_dispatch(phi, acc, m_s, z_s):
        phi_copy = pltpu.make_async_copy(phi_hbm, phi, phi_sem.at[0])
        phi_copy.start()
        pl.semaphore_wait(barrier, 3)
        for b in range(nb):
            send_x(b).start()
            send_y(b ^ 1).start()
        for b in range(nb):
            send_p(b).start()
        for e in range(RING):
            for c in weight_copies(e, e):
                c.start()
        xg[0, :, 0] = x_ref[...]
        g2 = scale_ref[0] * LOG2E
        phi_copy.wait()

        @pl.loop(0, n_slots // 512)
        def _(i):
            cols = pl.ds(pl.multiple_of(i * 512, 512), 512)
            v = phi[:, cols].astype(F32)
            phi[:, cols] = (v * lax.rsqrt(jnp.sum(v * v, axis=0, keepdims=True) + EPSILON)).astype(BF16)

        own = pl.ds(pl.multiple_of(s * (n_slots // 4) + d * slots, slots), slots)
        pnt[...] = phi[:, own].astype(F32).T.astype(BF16)

        @pl.loop(0, nb)
        def _(b):
            xn = unit_rows(x_ref[b].astype(F32))

            def chunk(i, carry):
                m, q = carry
                cols = pl.ds(pl.multiple_of(i * 512, 512), 512)
                lg = jnp.dot(xn, phi[:, cols], preferred_element_type=F32) * g2
                parts = [lg[:, 128 * k:128 * (k + 1)] for k in range(4)]
                m_new = jnp.maximum(m, jnp.maximum(jnp.maximum(parts[0], parts[1]), jnp.maximum(parts[2], parts[3])))
                e = [jnp.exp2(p - m_new) for p in parts]
                return m_new, q * jnp.exp2(m - m_new) + ((e[0] + e[1]) + (e[2] + e[3]))

            m, q = lax.fori_loop(0, n_slots // 512, chunk, (jnp.full((tok, 128), NEG_FILL, F32), jnp.zeros((tok, 128), F32)))
            big = jnp.max(m, axis=1, keepdims=True)
            tot = jnp.sum(q * jnp.exp2(m - big), axis=1, keepdims=True)
            pos = s * tok + lax.broadcasted_iota(jnp.int32, (1, tok), 1)
            rm[0, 0, pl.ds(b, 1), :] = row_of(big, tok)
            rm[0, 0, pl.ds(nb + b, 1), :] = jnp.where(pos < len_ref[b], 0.0, NEG_FILL)
            qrow[pl.ds(b, 1), :] = row_of(tot, tok)

        rm_x.start()
        rm_y.start()
        rm_p[0].start()

        def arrive(r, b):
            remote(xg.at[r, b, 0], xg.at[r, b, 0], sx_sem.at[0], r0_sem.at[4 * r + b], to_x).wait_recv()
            fwd_p(r, b).start()

        def unit(r, b, first):
            q = (r // 2) * nb + b
            remote(xg.at[r, b, 1], xg.at[r, b, 1], sp_sem.at[0], r1_sem.at[4 * r + b], to_p).wait_recv()
            xb = xg[r, b].reshape(2 * tok, dm)
            xn = unit_rows(xb.astype(F32))
            lt = lax.dot_general(pnt[...], xn, (((1,), (1,)), ((), ())), preferred_element_type=F32) * g2
            rmax = jnp.concatenate([rm[r, 0, pl.ds(b, 1), :], rm[r, 1, pl.ds(b, 1), :]], axis=1)
            mask = jnp.concatenate([rm[r, 0, pl.ds(nb + b, 1), :], rm[r, 1, pl.ds(nb + b, 1), :]], axis=1)
            ct[r, b] = jnp.exp2(lt - rmax).astype(BF16)
            lm = lt + mask
            mx = jnp.max(lm, axis=1, keepdims=True)
            if not first:
                m_old = m_s[q][:, 0:1]
                mx = jnp.maximum(mx, m_old)
            e = jnp.exp2(lm - mx)
            z = jnp.sum(e, axis=1, keepdims=True)
            part = jnp.dot(e.astype(BF16), xb, preferred_element_type=F32)
            if first:
                m_s[q] = jnp.broadcast_to(mx, (slots, 128))
                z_s[q] = jnp.broadcast_to(z, (slots, 128))
                acc[q] = part
            else:
                corr = jnp.exp2(m_old - mx)
                z = z + z_s[q][:, 0:1] * corr
                xs[q] = ((part + acc[q] * corr) / z).astype(BF16)

        remote(rm.at[0, 1], rm.at[0, 1], rms_sem.at[0], rm1_sem.at[0], to_p).wait_recv()

        @pl.loop(0, nb)
        def _(b):
            unit(0, b, True)

        for r, fwds in ((1, (rm_f, rm_p[1])), (2, (rm_p[2],))):
            remote(rm.at[r, 0], rm.at[r, 0], rms_sem.at[0], rm0_sem.at[r], to_x).wait_recv()
            for f in fwds:
                f.start()
        for r in (1, 2):
            remote(rm.at[r, 1], rm.at[r, 1], rms_sem.at[0], rm1_sem.at[r], to_p).wait_recv()

        @pl.loop(0, nb)
        def _(j):
            other = j + 1 - 2 * (j % 2)
            arrive(1, j)

            @pl.when(j % 2 == 0)
            def _():
                fwd_y(j).start()

            arrive(2, other)

            @pl.when(j % 2 == 0)
            def _():
                fwd_x(other).start()

            unit(1, j, False)
            unit(2, other, True)

        remote(rm.at[3, 0], rm.at[3, 0], rms_sem.at[0], rm0_sem.at[3], to_y).wait_recv()
        rm_p[3].start()
        remote(rm.at[3, 1], rm.at[3, 1], rms_sem.at[0], rm1_sem.at[3], to_p).wait_recv()

        @pl.loop(0, nb)
        def _(j):
            arrive(3, j)
            unit(3, j, False)

        for b in range(nb):
            send_x(b).wait_send()
            send_y(b).wait_send()
            send_p(b).wait_send()
            for r in (1, 2, 3):
                fwd_p(r, b).wait_send()
            (fwd_y(b) if b % 2 == 0 else fwd_x(b)).wait_send()
        for c in (rm_x, rm_y, rm_f, *rm_p):
            c.wait_send()

    pl.run_scoped(
        phase_dispatch,
        pltpu.VMEM((dm, n_slots), BF16),
        pltpu.VMEM((2 * nb, slots, dm), F32),
        pltpu.VMEM((2 * nb, slots, 128), F32),
        pltpu.VMEM((2 * nb, slots, 128), F32),
    )

    ff = w1b.shape[2]

    @pl.loop(0, n_exp)
    def _(e):
        slot = e % RING
        for c in weight_copies(e, slot):
            c.wait()
        rows = pl.ds(pl.multiple_of(e * 16, 16), 16)
        xe = xs[:, rows, :].reshape(2 * nb * 16, dm)
        total = jnp.zeros((2 * nb * 16, dm), F32)
        for k in range(0, ff, 512):
            h = jnp.dot(xe, w1b[slot, :, k:k + 512], preferred_element_type=F32)
            total += jnp.dot(gelu_tanh(h).astype(BF16), w2b[slot, k:k + 512, :], preferred_element_type=F32)
        xs[:, rows, :] = total.astype(BF16).reshape(2 * nb, 16, dm)

        @pl.when(e + RING < n_exp)
        def _():
            for c in weight_copies(e + RING, slot):
                c.start()

    def phase_combine(yst, d2s, stash):
        def d2_copy(r, b):
            return remote(d2s.at[r, b], d2r.at[r, b], d2s_sem.at[4 * r + b], d2r_sem.at[4 * r + b], to_p)

        def h_copy(b, odd):
            return remote(d2s.at[3, b], hr.at[b], hs_sem.at[b], hr_sem.at[b], to_y if odd else to_x)

        def f1_copy(b):
            return remote(d2s.at[1, b], f1r.at[b], f1s_sem.at[b], f1r_sem.at[b], to_x)

        def f2_copy(b):
            return remote(d2s.at[2, b], f2r.at[b], f2s_sem.at[b], f2r_sem.at[b], to_y)

        def comp(r, b, fresh):
            q = (r // 2) * nb + b
            if fresh:
                yst[q] = xs[q].astype(F32).T.astype(BF16)
            pt = jnp.dot(yst[q], ct[r, b], preferred_element_type=F32)
            d2s[r, b] = pt[:, tok:].astype(BF16)
            stash[r, b] = pt[:, :tok]
            d2_copy(r, b).start()

        def summed(r, b):
            d2_copy(r, b).wait()
            return stash[r, b] + d2r[r, b].astype(F32)

        @pl.loop(0, nb)
        def _(b):
            comp(3, b, True)

        @pl.loop(0, nb // 2)
        def _(j):
            b0, b1 = 2 * j, 2 * j + 1
            d2s[3, b0] = summed(3, b0).astype(BF16)
            h_copy(b0, False).start()
            d2s[3, b1] = summed(3, b1).astype(BF16)
            h_copy(b1, True).start()
            comp(1, b0, True)
            comp(2, b1, False)

        @pl.loop(0, nb // 2)
        def _(j):
            b0, b1 = 2 * j, 2 * j + 1
            d2s[1, b0] = summed(1, b0).astype(BF16)
            f1_copy(b0).start()
            d2s[2, b1] = summed(2, b1).astype(BF16)
            f2_copy(b1).start()
            comp(1, b1, True)
            comp(2, b0, False)

        @pl.loop(0, nb)
        def _(b):
            comp(0, b, False)

        @pl.loop(0, nb // 2)
        def _(j):
            b0, b1 = 2 * j, 2 * j + 1
            t1 = summed(1, b1)
            h_copy(b1, True).wait_recv()
            d2s[1, b1] = (t1 + hr[b1].astype(F32)).astype(BF16)
            f1_copy(b1).start()
            t2 = summed(2, b0)
            h_copy(b0, False).wait_recv()
            d2s[2, b0] = (t2 + hr[b0].astype(F32)).astype(BF16)
            f2_copy(b0).start()

        @pl.loop(0, nb)
        def _(b):
            t0 = summed(0, b)
            f1_copy(b).wait_recv()
            f2_copy(b).wait_recv()
            pos = s * tok + lax.broadcasted_iota(jnp.int32, (1, tok), 1)
            y = (t0 + f1r[b].astype(F32) + f2r[b].astype(F32)) / qrow[pl.ds(b, 1), :]
            y = jnp.where(pos < len_ref[b], y, 0.0)
            out_ref[b] = y.T.astype(BF16)

        for b in range(nb):
            h_copy(b, b % 2 == 1).wait_send()
            f1_copy(b).wait_send()
            f2_copy(b).wait_send()

    pl.run_scoped(
        phase_combine,
        pltpu.VMEM((2 * nb, dm, slots), BF16),
        pltpu.VMEM((4, nb, dm, tok), BF16),
        pltpu.VMEM((4, nb, dm, tok), F32),
    )


def solution(mesh):
    def local_layer(tok_blk, len_blk, slot_param, logit_scale, w_in, w_out):
        nb, tok, dm = tok_blk.shape
        n_slots = slot_param.shape[1]
        slots = n_slots // 8
        ff = w_in.shape[2]
        vmem = pl.BlockSpec(memory_space=pltpu.VMEM)
        smem = pl.BlockSpec(memory_space=pltpu.SMEM)
        hbm = pl.BlockSpec(memory_space=pl.ANY)
        dma = pltpu.SemaphoreType.DMA
        return pl.pallas_call(
            layer_kernel,
            out_shape=jax.ShapeDtypeStruct((nb, tok, dm), BF16),
            in_specs=[smem, smem, vmem, hbm, hbm, hbm],
            out_specs=vmem,
            scratch_shapes=[
                pltpu.VMEM((4, nb, 2, tok, dm), BF16),
                pltpu.VMEM((4, 2, 2 * nb, tok), F32),
                pltpu.VMEM((2 * nb, tok), F32),
                pltpu.VMEM((slots, dm), BF16),
                pltpu.VMEM((4, nb, slots, 2 * tok), BF16),
                pltpu.VMEM((2 * nb, slots, dm), BF16),
                pltpu.VMEM((4, nb, dm, tok), BF16),
                pltpu.VMEM((nb, dm, tok), BF16),
                pltpu.VMEM((nb, dm, tok), BF16),
                pltpu.VMEM((nb, dm, tok), BF16),
                pltpu.VMEM((RING, dm, ff), BF16),
                pltpu.VMEM((RING, ff, dm), BF16),
                dma((1,)), dma((RING,)), dma((RING,)),
                dma((nb,)), dma((nb,)), dma((4 * nb,)), dma((nb,)), dma((4 * nb,)), dma((4 * nb,)),
                dma((8,)), dma((4,)), dma((4,)),
                dma((4 * nb,)), dma((4 * nb,)), dma((nb,)), dma((nb,)), dma((nb,)), dma((nb,)), dma((nb,)), dma((nb,)),
            ],
            compiler_params=pltpu.CompilerParams(collective_id=0, has_side_effects=True, vmem_limit_bytes=67_000_000),
            name="soft_moe_layer",
        )(logit_scale.reshape(1), len_blk, tok_blk, slot_param, w_in, w_out)

    return jax.shard_map(local_layer, mesh=mesh, in_specs=(P("data", "seq", None), P("data"), P(None, None), P(), P("seq", None, None), P("seq", None, None)), out_specs=P("data", "seq", None), check_vma=False)
```

```python
import functools
import math

import jax
import jax.numpy as jnp
from jax import lax
from jax.experimental import pallas as pl
from jax.experimental.pallas import tpu as pltpu
from jax.sharding import PartitionSpec as P

EPSILON = 1e-6
NEG_FILL = -1e30
LOG2E = 1.0 / math.log(2.0)
F32 = jnp.float32
BF16 = jnp.bfloat16
RING = 10


def unit_rows(v32):
    return (v32 * lax.rsqrt(jnp.sum(v32 * v32, axis=1, keepdims=True) + EPSILON)).astype(BF16)


def gelu_tanh(h):
    inner = h * (math.sqrt(2.0 / math.pi) + (math.sqrt(2.0 / math.pi) * 0.044715) * (h * h))
    half = 0.5 * h
    return half + half * jnp.tanh(inner)


def row_of(col, rows):
    return jnp.broadcast_to(col, (rows, 128)).T[0:1, :]


def layer_kernel(
    scale_ref, len_ref, x_ref, phi_hbm, w1_hbm, w2_hbm, out_ref,
    xg, rm, rqs, rqr, wrow, pnt, ct, xs, d2r, hr, f1r, f2r, w1b, w2b,
    phi_sem, w1_sem, w2_sem,
    sx_sem, sy_sem, sp_sem, sf_sem, r0_sem, r1_sem,
    rms_sem, rm0_sem, rm1_sem, rqs_sem, rqr_sem,
    d2s_sem, d2r_sem, hs_sem, hr_sem, f1s_sem, f1r_sem, f2s_sem, f2r_sem,
):
    nb, tok, dm = x_ref.shape
    slots = pnt.shape[0]
    n_slots = phi_hbm.shape[1]
    n_exp = slots // 16
    d = lax.axis_index("data")
    s = lax.axis_index("seq")
    xc, core = s // 2, s % 2
    to_p = {"data": d, "seq": 2 * xc + (1 - core)}
    to_x = {"data": d, "seq": 2 * (1 - xc) + core}
    to_y = {"data": 1 - d, "seq": s}

    def remote(src, dst, send, recv, dev):
        return pltpu.make_async_remote_copy(src_ref=src, dst_ref=dst, send_sem=send, recv_sem=recv, device_id=dev, device_id_type=pl.DeviceIdType.MESH)

    def weight_copies(e, slot):
        return (
            pltpu.make_async_copy(w1_hbm.at[n_exp * d + e], w1b.at[slot], w1_sem.at[slot]),
            pltpu.make_async_copy(w2_hbm.at[n_exp * d + e], w2b.at[slot], w2_sem.at[slot]),
        )

    barrier = pltpu.get_barrier_semaphore()
    for dev in (to_p, to_x, to_y):
        pl.semaphore_signal(barrier, inc=1, device_id=dev, device_id_type=pl.DeviceIdType.MESH)

    def send_x(b):
        return remote(x_ref.at[b], xg.at[1, b, 0], sx_sem.at[b], r0_sem.at[4 + b], to_x)

    def send_y(b):
        return remote(x_ref.at[b], xg.at[2, b, 0], sy_sem.at[b], r0_sem.at[8 + b], to_y)

    def send_p(b):
        return remote(x_ref.at[b], xg.at[0, b, 1], sp_sem.at[b], r1_sem.at[b], to_p)

    def fwd_p(r, b):
        return remote(xg.at[r, b, 0], xg.at[r, b, 1], sp_sem.at[4 * r + b], r1_sem.at[4 * r + b], to_p)

    def fwd_y(b):
        return remote(xg.at[1, b, 0], xg.at[3, b, 0], sf_sem.at[b], r0_sem.at[12 + b], to_y)

    def fwd_x(b):
        return remote(xg.at[2, b, 0], xg.at[3, b, 0], sf_sem.at[b], r0_sem.at[12 + b], to_x)

    rm_x = remote(rm.at[0, 0], rm.at[1, 0], rms_sem.at[0], rm0_sem.at[1], to_x)
    rm_y = remote(rm.at[0, 0], rm.at[2, 0], rms_sem.at[1], rm0_sem.at[2], to_y)
    rm_f = remote(rm.at[1, 0], rm.at[3, 0], rms_sem.at[2], rm0_sem.at[3], to_y)
    rm_p = [remote(rm.at[r, 0], rm.at[r, 1], rms_sem.at[3 + r], rm1_sem.at[r], to_p) for r in range(4)]

    def phase_dispatch(phi, acc, m_s, z_s):
        own = pl.ds(pl.multiple_of(s * (n_slots // 4) + d * slots, slots), slots)
        phi_copy = pltpu.make_async_copy(phi_hbm.at[:, own], phi, phi_sem.at[0])
        phi_copy.start()
        pos = s * tok + lax.broadcasted_iota(jnp.int32, (1, tok), 1)
        for b in range(nb):
            rm[0, 0, b:b + 1, :] = jnp.where(pos < len_ref[b], 0.0, NEG_FILL)
        pl.semaphore_wait(barrier, 3)
        rm_x.start()
        rm_y.start()
        rm_p[0].start()
        for b in range(nb):
            send_x(b).start()
            send_y(b ^ 1).start()
        for b in range(nb):
            send_p(b).start()
        for e in range(RING):
            for c in weight_copies(e, e):
                c.start()
        xg[0, :, 0] = x_ref[...]
        g2 = scale_ref[0] * LOG2E
        phi_copy.wait()
        v = phi[...].astype(F32)
        pnt[...] = (v * lax.rsqrt(jnp.sum(v * v, axis=0, keepdims=True) + EPSILON)).T.astype(BF16)
        for r, fwds in ((1, (rm_f, rm_p[1])), (2, (rm_p[2],))):
            remote(rm.at[r, 0], rm.at[r, 0], rms_sem.at[0], rm0_sem.at[r], to_x).wait_recv()
            for f in fwds:
                f.start()

        def arrive(r, b):
            remote(xg.at[r, b, 0], xg.at[r, b, 0], sx_sem.at[0], r0_sem.at[4 * r + b], to_x).wait_recv()
            fwd_p(r, b).start()

        def wait_partner(r, b):
            remote(xg.at[r, b, 1], xg.at[r, b, 1], sp_sem.at[0], r1_sem.at[4 * r + b], to_p).wait_recv()

        def wait_mask(r):
            remote(rm.at[r, 1], rm.at[r, 1], rms_sem.at[0], rm1_sem.at[r], to_p).wait_recv()

        def unit(r, b, first):
            q = (r // 2) * nb + b
            xb = xg[r, b].reshape(2 * tok, dm)
            xn = unit_rows(xb.astype(F32))
            lt = lax.dot_general(pnt[...], xn, (((1,), (1,)), ((), ())), preferred_element_type=F32) * g2
            mask = jnp.concatenate([rm[r, 0, pl.ds(b, 1), :], rm[r, 1, pl.ds(b, 1), :]], axis=1)
            lm = lt + mask
            mx = jnp.broadcast_to(jnp.max(lm, axis=1, keepdims=True), (slots, 128))
            if not first:
                m_old = m_s[q]
                mx = jnp.maximum(mx, m_old)
            e = jnp.exp2(lm - jnp.concatenate([mx] * 4, axis=1))
            z = (e[:, 0:128] + e[:, 128:256]) + (e[:, 256:384] + e[:, 384:512])
            part = jnp.dot(e.astype(BF16), xb, preferred_element_type=F32)
            cmax = jnp.max(lt, axis=0, keepdims=True)
            c = jnp.exp2(lt - cmax)
            rqs[0, r, pl.ds(b, 1), :] = cmax
            rqs[0, r, pl.ds(nb + b, 1), :] = jnp.sum(c, axis=0, keepdims=True)
            ct[r, b] = c.astype(BF16)
            if first:
                m_s[q] = mx
                z_s[q] = z
                acc[q] = part
            else:
                corr = jnp.exp2(m_old - mx)
                z = jnp.broadcast_to(jnp.sum(z + z_s[q] * corr, axis=1, keepdims=True), (slots, 128))
                inv = 1.0 / z
                xs[q] = ((part + acc[q] * jnp.concatenate([corr] * 3, axis=1)) * jnp.concatenate([inv] * 3, axis=1)).astype(BF16)

        wait_mask(0)

        @pl.loop(0, nb)
        def _(b):
            wait_partner(0, b)
            unit(0, b, True)

        for r in (1, 2):
            wait_mask(r)

        @pl.loop(0, nb)
        def _(j):
            other = j + 1 - 2 * (j % 2)
            arrive(1, j)
            arrive(2, other)

            @pl.when(j % 2 == 0)
            def _():
                fwd_y(j).start()
                fwd_x(other).start()

            wait_partner(1, j)
            wait_partner(2, other)
            unit(1, j, False)
            unit(2, other, True)

        remote(rm.at[3, 0], rm.at[3, 0], rms_sem.at[0], rm0_sem.at[3], to_y).wait_recv()
        rm_p[3].start()
        wait_mask(3)

        @pl.loop(0, nb // 2)
        def _(j):
            for b in (2 * j, 2 * j + 1):
                arrive(3, b)
            for b in (2 * j, 2 * j + 1):
                wait_partner(3, b)
            for b in (2 * j, 2 * j + 1):
                unit(3, b, False)

        for b in range(nb):
            send_x(b).wait_send()
            send_y(b).wait_send()
            send_p(b).wait_send()
            for r in (1, 2, 3):
                fwd_p(r, b).wait_send()
            (fwd_y(b) if b % 2 == 0 else fwd_x(b)).wait_send()
        for c in (rm_x, rm_y, rm_f, *rm_p):
            c.wait_send()

    pl.run_scoped(
        phase_dispatch,
        pltpu.VMEM((dm, slots), BF16),
        pltpu.VMEM((2 * nb, slots, dm), F32),
        pltpu.VMEM((2 * nb, slots, 128), F32),
        pltpu.VMEM((2 * nb, slots, 128), F32),
    )

    rq_copies = [remote(rqs.at[k], rqr.at[k], rqs_sem.at[k], rqr_sem.at[k], dev) for k, dev in enumerate((to_p, to_x, to_y))]

    def merge(k):
        rq_copies[k].wait()
        for r in range(4):
            if k == 0:
                theirs = jnp.concatenate([rqr[k, r][:, tok:], rqr[k, r][:, :tok]], axis=1)
            else:
                theirs = rqr[k, r ^ k]
            mine = rqs[k, r]
            top = jnp.maximum(mine[:nb], theirs[:nb])
            low = mine[nb:] * jnp.exp2(mine[:nb] - top) + theirs[nb:] * jnp.exp2(theirs[:nb] - top)
            rqs[k + 1, r, :nb] = top
            rqs[k + 1, r, nb:] = low
            if k == 2:
                wrow[r] = jnp.exp2(rqs[0, r][:nb] - top)
        if k < 2:
            rq_copies[k + 1].start()

    rq_copies[0].start()

    def ffn_pair(i):
        pair = (2 * i, 2 * i + 1)
        for e in pair:
            for c in weight_copies(e, e % RING):
                c.wait()
        rows = [pl.ds(pl.multiple_of(e * 16, 16), 16) for e in pair]
        xe = [xs[:, r, :].reshape(2 * nb * 16, dm) for r in rows]
        hs = [jnp.dot(x, w1b[e % RING], preferred_element_type=F32) for x, e in zip(xe, pair)]
        ys = [jnp.dot(gelu_tanh(h).astype(BF16), w2b[e % RING], preferred_element_type=F32) for h, e in zip(hs, pair)]
        for y, r in zip(ys, rows):
            xs[:, r, :] = y.astype(BF16).reshape(2 * nb, 16, dm)
        for e in pair:
            @pl.when(e + RING < n_exp)
            def _():
                for c in weight_copies(e + RING, e % RING):
                    c.start()

    @pl.loop(0, n_exp // 2)
    def _(i):
        ffn_pair(i)
        for k in range(3):
            @pl.when(i == 4 * (k + 1))
            def _():
                merge(k)

    def phase_combine(yst, d2s, stash):
        def d2_copy(r, b):
            return remote(d2s.at[r, b], d2r.at[r, b], d2s_sem.at[4 * r + b], d2r_sem.at[4 * r + b], to_p)

        def h_copy(b, odd):
            return remote(d2s.at[3, b], hr.at[b], hs_sem.at[b], hr_sem.at[b], to_y if odd else to_x)

        def f1_copy(b):
            return remote(d2s.at[1, b], f1r.at[b], f1s_sem.at[b], f1r_sem.at[b], to_x)

        def f2_copy(b):
            return remote(d2s.at[2, b], f2r.at[b], f2s_sem.at[b], f2r_sem.at[b], to_y)

        def comp(r, b, fresh):
            q = (r // 2) * nb + b
            if fresh:
                yst[q] = xs[q].astype(F32).T.astype(BF16)
            pt = jnp.dot(yst[q], ct[r, b], preferred_element_type=F32)
            pt = pt * wrow[r, pl.ds(b, 1), :]
            d2s[r, b] = pt[:, tok:].astype(BF16)
            stash[r, b] = pt[:, :tok]
            d2_copy(r, b).start()

        def summed(r, b):
            d2_copy(r, b).wait()
            return stash[r, b] + d2r[r, b].astype(F32)

        @pl.loop(0, nb)
        def _(b):
            comp(3, b, True)

        @pl.loop(0, nb // 2)
        def _(j):
            b0, b1 = 2 * j, 2 * j + 1
            d2s[3, b0] = summed(3, b0).astype(BF16)
            h_copy(b0, False).start()
            d2s[3, b1] = summed(3, b1).astype(BF16)
            h_copy(b1, True).start()
            comp(1, b0, True)
            comp(2, b1, False)

        @pl.loop(0, nb // 2)
        def _(j):
            b0, b1 = 2 * j, 2 * j + 1
            d2s[1, b0] = summed(1, b0).astype(BF16)
            f1_copy(b0).start()
            d2s[2, b1] = summed(2, b1).astype(BF16)
            f2_copy(b1).start()
            comp(1, b1, True)
            comp(2, b0, False)

        @pl.loop(0, nb)
        def _(b):
            comp(0, b, False)

        @pl.loop(0, nb // 2)
        def _(j):
            b0, b1 = 2 * j, 2 * j + 1
            t1 = summed(1, b1)
            h_copy(b1, True).wait_recv()
            d2s[1, b1] = (t1 + hr[b1].astype(F32)).astype(BF16)
            f1_copy(b1).start()
            t2 = summed(2, b0)
            h_copy(b0, False).wait_recv()
            d2s[2, b0] = (t2 + hr[b0].astype(F32)).astype(BF16)
            f2_copy(b0).start()

        @pl.loop(0, nb)
        def _(b):
            t0 = summed(0, b)
            f1_copy(b).wait_recv()
            f2_copy(b).wait_recv()
            pos = s * tok + lax.broadcasted_iota(jnp.int32, (1, tok), 1)
            y = (t0 + f1r[b].astype(F32) + f2r[b].astype(F32)) / rqs[3, 0, pl.ds(nb + b, 1), :tok]
            y = jnp.where(pos < len_ref[b], y, 0.0)
            out_ref[b] = y.T.astype(BF16)

        for b in range(nb):
            h_copy(b, b % 2 == 1).wait_send()
            f1_copy(b).wait_send()
            f2_copy(b).wait_send()

    pl.run_scoped(
        phase_combine,
        pltpu.VMEM((2 * nb, dm, slots), BF16),
        pltpu.VMEM((4, nb, dm, tok), BF16),
        pltpu.VMEM((4, nb, dm, tok), F32),
    )


def solution(mesh):
    def local_layer(tok_blk, len_blk, slot_param, logit_scale, w_in, w_out):
        nb, tok, dm = tok_blk.shape
        n_slots = slot_param.shape[1]
        slots = n_slots // 8
        ff = w_in.shape[2]
        vmem = pl.BlockSpec(memory_space=pltpu.VMEM)
        smem = pl.BlockSpec(memory_space=pltpu.SMEM)
        hbm = pl.BlockSpec(memory_space=pl.ANY)
        dma = pltpu.SemaphoreType.DMA
        return pl.pallas_call(
            layer_kernel,
            out_shape=jax.ShapeDtypeStruct((nb, tok, dm), BF16),
            in_specs=[smem, smem, vmem, hbm, hbm, hbm],
            out_specs=vmem,
            scratch_shapes=[
                pltpu.VMEM((4, nb, 2, tok, dm), BF16),
                pltpu.VMEM((4, 2, nb, tok), F32),
                pltpu.VMEM((4, 4, 2 * nb, 2 * tok), F32),
                pltpu.VMEM((3, 4, 2 * nb, 2 * tok), F32),
                pltpu.VMEM((4, nb, 2 * tok), F32),
                pltpu.VMEM((slots, dm), BF16),
                pltpu.VMEM((4, nb, slots, 2 * tok), BF16),
                pltpu.VMEM((2 * nb, slots, dm), BF16),
                pltpu.VMEM((4, nb, dm, tok), BF16),
                pltpu.VMEM((nb, dm, tok), BF16),
                pltpu.VMEM((nb, dm, tok), BF16),
                pltpu.VMEM((nb, dm, tok), BF16),
                pltpu.VMEM((RING, dm, ff), BF16),
                pltpu.VMEM((RING, ff, dm), BF16),
                dma((1,)), dma((RING,)), dma((RING,)),
                dma((nb,)), dma((nb,)), dma((4 * nb,)), dma((nb,)), dma((4 * nb,)), dma((4 * nb,)),
                dma((8,)), dma((4,)), dma((4,)), dma((3,)), dma((3,)),
                dma((4 * nb,)), dma((4 * nb,)), dma((nb,)), dma((nb,)), dma((nb,)), dma((nb,)), dma((nb,)), dma((nb,)),
            ],
            compiler_params=pltpu.CompilerParams(collective_id=0, has_side_effects=True, vmem_limit_bytes=67_000_000),
            name="soft_moe_layer",
        )(logit_scale.reshape(1), len_blk, tok_blk, slot_param, w_in, w_out)

    return jax.shard_map(local_layer, mesh=mesh, in_specs=(P("data", "seq", None), P("data"), P(None, None), P(), P("seq", None, None), P("seq", None, None)), out_specs=P("data", "seq", None), check_vma=False)
```

```python
import functools
import math

import jax
import jax.numpy as jnp
from jax import lax
from jax.experimental import pallas as pl
from jax.experimental.pallas import tpu as pltpu
from jax.sharding import PartitionSpec as P

EPSILON = 1e-6
NEG_FILL = -1e30
LOG2E = 1.0 / math.log(2.0)
F32 = jnp.float32
BF16 = jnp.bfloat16
RING = 14


def unit_rows(v32):
    return (v32 * lax.rsqrt(jnp.sum(v32 * v32, axis=1, keepdims=True) + EPSILON)).astype(BF16)


def gelu_tanh(h):
    inner = h * (math.sqrt(2.0 / math.pi) + (math.sqrt(2.0 / math.pi) * 0.044715) * (h * h))
    half = 0.5 * h
    return half + half * jnp.tanh(inner)


def row_of(col, rows):
    return jnp.broadcast_to(col, (rows, 128)).T[0:1, :]


def layer_kernel(
    scale_hbm, len_hbm, x_hbm, phi_hbm, w1_hbm, w2_hbm, out_ref,
    scale_ref, len_ref, xg, rm, rqs, rqr, wrow, ct, xs, d2r, hr, f1r, f2r, w1b, w2b,
    in_sem, w_sem, send_sem, r0_sem, r1_sem, rms_sem, rmr_sem, rqs_sem, rqr_sem, d2s_sem,
):
    nb, tok, dm = x_hbm.shape
    slots = xs.shape[1]
    n_slots = phi_hbm.shape[1]
    n_exp = slots // 16
    d = lax.axis_index("data")
    s = lax.axis_index("seq")
    xc, core = s // 2, s % 2
    to_p = {"data": d, "seq": 2 * xc + (1 - core)}
    to_x = {"data": d, "seq": 2 * (1 - xc) + core}
    to_y = {"data": 1 - d, "seq": s}

    def remote(src, dst, send, recv, dev):
        return pltpu.make_async_remote_copy(src_ref=src, dst_ref=dst, send_sem=send, recv_sem=recv, device_id=dev, device_id_type=pl.DeviceIdType.MESH)

    def weight_copies(e, slot):
        return (
            pltpu.make_async_copy(w1_hbm.at[n_exp * d + e], w1b.at[slot], w_sem.at[slot]),
            pltpu.make_async_copy(w2_hbm.at[n_exp * d + e], w2b.at[slot], w_sem.at[slot]),
        )

    barrier = pltpu.get_barrier_semaphore()
    for dev in (to_p, to_x, to_y):
        pl.semaphore_signal(barrier, inc=1, device_id=dev, device_id_type=pl.DeviceIdType.MESH)

    phi = ct.at[3, nb - 1, 0:dm]
    pnt = xs.at[2 * nb - 1]
    loads = [
        pltpu.make_async_copy(x_hbm, xg.at[0, :, 0], in_sem.at[0]),
        pltpu.make_async_copy(phi_hbm.at[:, pl.ds(pl.multiple_of(s * (n_slots // 4) + d * slots, slots), slots)], phi, in_sem.at[1]),
        pltpu.make_async_copy(len_hbm, len_ref, in_sem.at[2]),
        pltpu.make_async_copy(scale_hbm, scale_ref, in_sem.at[3]),
    ]
    for c in loads:
        c.start()

    by_x, by_y, by_p = send_sem.at[0], send_sem.at[1], send_sem.at[2]

    def blocks(ref, sem):
        return pltpu.make_async_copy(ref, ref, sem)

    def send_x(b):
        return remote(xg.at[0, b, 0], xg.at[1, b, 0], by_x, r0_sem.at[b], to_x)

    def send_y(b):
        return remote(xg.at[0, b, 0], xg.at[2, b, 0], by_y, r0_sem.at[b ^ 1], to_y)

    def send_p(b):
        return remote(xg.at[0, b, 0], xg.at[0, b, 1], by_p, r1_sem.at[b], to_p)

    half = tok // 2

    def fwd_across(r, b, h, send, dev):
        part = slice(h * half, (h + 1) * half)
        return remote(xg.at[r, b, 0, part], xg.at[3, b, 0, part], send, r0_sem.at[4 + 2 * (b // 2) + h], dev)

    def arrive_pair(j):
        other = j + 1 - 2 * (j % 2)
        blocks(xg.at[0, 0], r0_sem.at[j]).wait()
        for r, b in ((1, j), (2, other)):
            remote(xg.at[r, b, 0], xg.at[r, b, 1], by_p, r1_sem.at[nb + j], to_p).start()

        @pl.when(j % 2 == 0)
        def _():
            for h in range(2):
                fwd_across(1, j, h, by_y, to_y).start()
                fwd_across(2, other, h, by_x, to_x).start()

    def arrive_across(j, h):
        part = slice(h * half, (h + 1) * half)
        blocks(xg.at[0, 0, 0], r0_sem.at[4 + 2 * j + h]).wait()
        for b in (2 * j, 2 * j + 1):
            remote(xg.at[3, b, 0, part], xg.at[3, b, 1, part], by_p, r1_sem.at[2 * nb + j], to_p).start()

    rm_x = remote(rm.at[0, 0], rm.at[1, 0], rms_sem.at[0], rmr_sem.at[0], to_x)
    rm_y = remote(rm.at[0, 0], rm.at[2, 0], rms_sem.at[0], rmr_sem.at[0], to_y)
    rm_f = remote(rm.at[1, 0], rm.at[3, 0], rms_sem.at[0], rmr_sem.at[1], to_y)
    rm_p = [remote(rm.at[r, 0], rm.at[r, 1], rms_sem.at[1], rmr_sem.at[(2, 3, 3, 4)[r]], to_p) for r in range(4)]

    def phase_dispatch(acc, m_s, z_s):
        loads[2].wait()
        pos = s * tok + lax.broadcasted_iota(jnp.int32, (1, tok), 1)
        for b in range(nb):
            rm[0, 0, b:b + 1, :] = jnp.where(pos < len_ref[b], 0.0, NEG_FILL)
        loads[0].wait()
        pl.semaphore_wait(barrier, 3)
        rm_x.start()
        rm_y.start()
        rm_p[0].start()
        for b in range(nb):
            send_x(b).start()
            send_y(b ^ 1).start()
        for b in range(nb):
            send_p(b).start()
        for e in range(RING):
            for c in weight_copies(e, e):
                c.start()
        loads[3].wait()
        g2 = scale_ref[0] * LOG2E
        loads[1].wait()
        v = phi[...].astype(F32)
        pnt[...] = (v * lax.rsqrt(jnp.sum(v * v, axis=0, keepdims=True) + EPSILON)).T.astype(BF16)
        blocks(rm.at[0], rmr_sem.at[0]).wait()
        for c in (rm_f, rm_p[1], rm_p[2]):
            c.start()

        def unit(r, b, first, last):
            q = (r // 2) * nb + b
            a = b if r < 2 else b + 1 - 2 * (b % 2)
            xb = xg[r, b].reshape(2 * tok, dm)
            xn = unit_rows(xb.astype(F32))
            lt = lax.dot_general(pnt[...], xn, (((1,), (1,)), ((), ())), preferred_element_type=F32) * g2
            lm = lt + jnp.concatenate([rm[r, k, pl.ds(b, 1), :] for k in range(2)], axis=1)
            mx = jnp.broadcast_to(jnp.max(lm, axis=1, keepdims=True), (slots, 128))
            if not first:
                m_old = m_s[a]
                mx = jnp.maximum(mx, m_old)
            e = jnp.exp2(lm - jnp.concatenate([mx] * 4, axis=1))
            z = (e[:, 0:128] + e[:, 128:256]) + (e[:, 256:384] + e[:, 384:512])
            part = jnp.dot(e.astype(BF16), xb, preferred_element_type=F32)
            cmax = jnp.max(lt, axis=0, keepdims=True)
            c = jnp.exp2(lt - cmax)
            rqs[0, r, pl.ds(b, 1), :] = cmax
            rqs[0, r, pl.ds(nb + b, 1), :] = jnp.sum(c, axis=0, keepdims=True)
            ct[r, b] = c.astype(BF16)
            if not first:
                corr = jnp.exp2(m_old - mx)
                z = z + z_s[a] * corr
                part = part + acc[a] * jnp.concatenate([corr] * 3, axis=1)
            if last:
                inv = 1.0 / jnp.broadcast_to(jnp.sum(z, axis=1, keepdims=True), (slots, 128))
                xs[q] = (part * jnp.concatenate([inv] * 3, axis=1)).astype(BF16)
            else:
                m_s[a] = mx
                z_s[a] = z
                acc[a] = part

        blocks(rm.at[0, 0], rmr_sem.at[2]).wait()

        @pl.loop(0, nb)
        def _(b):
            blocks(xg.at[0, 0, 0], r1_sem.at[b]).wait()
            unit(0, b, True, False)

        arrive_pair(0)
        blocks(rm.at[0], rmr_sem.at[3]).wait()

        @pl.loop(0, nb)
        def _(j):
            blocks(xg.at[0, 0], r1_sem.at[nb + j]).wait()
            unit(1, j, False, True)

            @pl.when(j < nb - 1)
            def _():
                arrive_pair(j + 1)

            unit(2, j + 1 - 2 * (j % 2), True, False)

        blocks(rm.at[0, 0], rmr_sem.at[1]).wait()
        rm_p[3].start()
        for h in range(2):
            arrive_across(0, h)
        blocks(rm.at[0, 0], rmr_sem.at[4]).wait()

        @pl.loop(0, nb // 2)
        def _(j):
            blocks(xg.at[0, 0], r1_sem.at[2 * nb + j]).wait()
            unit(3, 2 * j, False, True)

            @pl.when(j < nb // 2 - 1)
            def _():
                arrive_across(j + 1, 0)

            unit(3, 2 * j + 1, False, True)

            @pl.when(j < nb // 2 - 1)
            def _():
                arrive_across(j + 1, 1)

        blocks(xg.at[0, 0:3], by_x).wait()
        blocks(xg.at[0, 0:3], by_y).wait()
        blocks(xg.at[0:2], by_p).wait()
        blocks(rm.at[0:3, 0], rms_sem.at[0]).wait()
        blocks(rm.at[0:2], rms_sem.at[1]).wait()

    pl.run_scoped(
        phase_dispatch,
        pltpu.VMEM((nb, slots, dm), F32),
        pltpu.VMEM((nb, slots, 128), F32),
        pltpu.VMEM((nb, slots, 128), F32),
    )

    rq_copies = [remote(rqs.at[k], rqr.at[k], rqs_sem.at[0], rqr_sem.at[k], dev) for k, dev in enumerate((to_p, to_x, to_y))]

    def merge(k):
        rq_copies[k].wait()
        for r in range(4):
            if k == 0:
                theirs = jnp.concatenate([rqr[k, r][:, tok:], rqr[k, r][:, :tok]], axis=1)
            else:
                theirs = rqr[k, r ^ k]
            mine = rqs[k, r]
            top = jnp.maximum(mine[:nb], theirs[:nb])
            low = mine[nb:] * jnp.exp2(mine[:nb] - top) + theirs[nb:] * jnp.exp2(theirs[:nb] - top)
            rqs[k + 1, r, :nb] = top
            rqs[k + 1, r, nb:] = low
            if k == 2:
                wrow[r] = jnp.exp2(rqs[0, r][:nb] - top)
        if k < 2:
            rq_copies[k + 1].start()

    rq_copies[0].start()

    def ffn(es):
        for e in es:
            blocks(w1b.at[0:2], w_sem.at[e % RING]).wait()
        rows = [pl.ds(pl.multiple_of(e * 16, 16), 16) for e in es]
        xe = [xs[:, r, :].reshape(2 * nb * 16, dm) for r in rows]
        hs = [jnp.dot(x, w1b[e % RING], preferred_element_type=F32) for x, e in zip(xe, es)]
        ys = [jnp.dot(gelu_tanh(h).astype(BF16), w2b[e % RING], preferred_element_type=F32) for h, e in zip(hs, es)]
        for y, r in zip(ys, rows):
            xs[:, r, :] = y.astype(BF16).reshape(2 * nb, 16, dm)
        for e in es:
            @pl.when(e + RING < n_exp)
            def _():
                for c in weight_copies(e + RING, e % RING):
                    c.start()

    ffn([0, 1])

    @pl.loop(0, (n_exp - 4) // 4)
    def _(i):
        ffn([4 * i + 2 + k for k in range(4)])
        for k in range(3):
            @pl.when(i == 2 * k + 1)
            def _():
                merge(k)

    ffn([n_exp - 2, n_exp - 1])

    def phase_combine(d2s, stash):
        def d2_start(r, b, g):
            remote(d2s.at[r, b], d2r.at[r, b], d2s_sem.at[g], r1_sem.at[g], to_p).start()

        def d2_wait(g, count):
            blocks(d2s.at[0, 0:count], d2s_sem.at[g]).wait()
            blocks(d2r.at[0, 0:count], r1_sem.at[g]).wait()

        def half_sum(r, b, cols):
            yt = xs[(r // 2) * nb + b].astype(F32).T.astype(BF16)
            return jnp.dot(yt, ct[r, b, :, cols], preferred_element_type=F32) * wrow[r, pl.ds(b, 1), :][:, cols]

        def comp(r, b, g):
            d2s[r, b] = half_sum(r, b, slice(tok, 2 * tok)).astype(BF16)
            d2_start(r, b, g)

        def mine(r, b):
            return half_sum(r, b, slice(0, tok))

        def h_start(b, odd):
            send, dev = (by_y, to_y) if odd else (by_x, to_x)
            remote(d2s.at[3, b], hr.at[b], send, r0_sem.at[b // 2], dev).start()

        def f1_start(b):
            remote(d2s.at[1, b], f1r.at[b], by_x, r0_sem.at[nb + b], to_x).start()

        def f2_start(b):
            remote(d2s.at[2, b], f2r.at[b], by_y, r0_sem.at[nb + b], to_y).start()

        @pl.loop(0, nb)
        def _(b):
            comp(3, b, b // 2)

        @pl.loop(0, nb // 2)
        def _(j):
            b0, b1 = 2 * j, 2 * j + 1
            t0 = mine(3, b0)
            d2_wait(j, 2)
            d2s[3, b0] = (t0 + d2r[3, b0].astype(F32)).astype(BF16)
            h_start(b0, False)
            d2s[3, b1] = (mine(3, b1) + d2r[3, b1].astype(F32)).astype(BF16)
            h_start(b1, True)
            comp(1, b0, 2 + j)
            comp(2, b1, 2 + j)

        @pl.loop(0, nb // 2)
        def _(j):
            b0, b1 = 2 * j, 2 * j + 1
            d2_wait(2 + j, 2)
            d2s[1, b0] = (mine(1, b0) + d2r[1, b0].astype(F32)).astype(BF16)
            f1_start(b0)
            d2s[2, b1] = (mine(2, b1) + d2r[2, b1].astype(F32)).astype(BF16)
            f2_start(b1)
            comp(1, b1, 4 + j)
            comp(2, b0, 4 + j)

        @pl.loop(0, nb // 2)
        def _(j):
            b0, b1 = 2 * j, 2 * j + 1
            t1, t2 = mine(1, b1), mine(2, b0)
            d2_wait(4 + j, 2)
            t1 += d2r[1, b1].astype(F32)
            t2 += d2r[2, b0].astype(F32)
            blocks(hr.at[0:2], r0_sem.at[j]).wait()
            d2s[1, b1] = (t1 + hr[b1].astype(F32)).astype(BF16)
            f1_start(b1)
            d2s[2, b0] = (t2 + hr[b0].astype(F32)).astype(BF16)
            f2_start(b0)

        @pl.loop(0, nb)
        def _(b):
            comp(0, b, 6)

        @pl.loop(0, nb)
        def _(b):
            stash[b] = mine(0, b)

        d2_wait(6, nb)

        @pl.loop(0, nb)
        def _(b):
            base = stash[b] + d2r[0, b].astype(F32)
            blocks(f1r.at[0:2], r0_sem.at[nb + b]).wait()
            pos = s * tok + lax.broadcasted_iota(jnp.int32, (1, tok), 1)
            y = (base + f1r[b].astype(F32) + f2r[b].astype(F32)) / rqs[3, 0, pl.ds(nb + b, 1), :tok]
            y = jnp.where(pos < len_ref[b], y, 0.0)
            out_ref[b] = y.T.astype(BF16)

        blocks(xg.at[0, 0:3], by_x).wait()
        blocks(xg.at[0, 0:3], by_y).wait()

    pl.run_scoped(
        phase_combine,
        pltpu.VMEM((4, nb, dm, tok), BF16),
        pltpu.VMEM((nb, dm, tok), F32),
    )


def solution(mesh):
    def local_layer(tok_blk, len_blk, slot_param, logit_scale, w_in, w_out):
        nb, tok, dm = tok_blk.shape
        n_slots = slot_param.shape[1]
        slots = n_slots // 8
        ff = w_in.shape[2]
        hbm = pl.BlockSpec(memory_space=pl.ANY)
        dma = pltpu.SemaphoreType.DMA
        return pl.pallas_call(
            layer_kernel,
            out_shape=pltpu.VMEM((nb, tok, dm), BF16),
            in_specs=[hbm] * 6,
            out_specs=pl.BlockSpec(memory_space=pltpu.VMEM),
            scratch_shapes=[
                pltpu.SMEM((1,), F32),
                pltpu.SMEM((nb,), jnp.int32),
                pltpu.VMEM((4, nb, 2, tok, dm), BF16),
                pltpu.VMEM((4, 2, nb, tok), F32),
                pltpu.VMEM((4, 4, 2 * nb, 2 * tok), F32),
                pltpu.VMEM((3, 4, 2 * nb, 2 * tok), F32),
                pltpu.VMEM((4, nb, 2 * tok), F32),
                pltpu.VMEM((4, nb, slots, 2 * tok), BF16),
                pltpu.VMEM((2 * nb, slots, dm), BF16),
                pltpu.VMEM((4, nb, dm, tok), BF16),
                pltpu.VMEM((nb, dm, tok), BF16),
                pltpu.VMEM((nb, dm, tok), BF16),
                pltpu.VMEM((nb, dm, tok), BF16),
                pltpu.VMEM((RING, dm, ff), BF16),
                pltpu.VMEM((RING, ff, dm), BF16),
                dma((4,)), dma((RING,)), dma((3,)), dma((2 * nb,)), dma((2 * nb + 2,)), dma((2,)), dma((5,)), dma((1,)), dma((3,)), dma((7,)),
            ],
            compiler_params=pltpu.CompilerParams(collective_id=0, has_side_effects=True, vmem_limit_bytes=66_250_000),
            name="soft_moe_layer",
        )(logit_scale.reshape(1), len_blk, tok_blk, slot_param, w_in, w_out)

    return jax.shard_map(local_layer, mesh=mesh, in_specs=(P("data", "seq", None), P("data"), P(None, None), P(), P("seq", None, None), P("seq", None, None)), out_specs=P("data", "seq", None), check_vma=False)
```

```python
import functools
import math

import jax
import jax.numpy as jnp
from jax import lax
from jax.experimental import pallas as pl
from jax.experimental.pallas import tpu as pltpu
from jax.sharding import PartitionSpec as P

EPSILON = 1e-6
NEG_FILL = -1e30
LOG2E = 1.0 / math.log(2.0)
F32 = jnp.float32
BF16 = jnp.bfloat16
RING = 14


def unit_rows(v32):
    return (v32 * lax.rsqrt(jnp.sum(v32 * v32, axis=1, keepdims=True) + EPSILON)).astype(BF16)


def gelu_tanh(h):
    inner = h * (math.sqrt(2.0 / math.pi) + (math.sqrt(2.0 / math.pi) * 0.044715) * (h * h))
    half = 0.5 * h
    return half + half * jnp.tanh(inner)


def row_of(col, rows):
    return jnp.broadcast_to(col, (rows, 128)).T[0:1, :]


def layer_kernel(
    scale_hbm, len_hbm, x_hbm, phi_hbm, w1_hbm, w2_hbm, out_ref,
    scale_ref, len_ref, xg, rm, rqs, rqr, wrow, ct, xs, d2r, hr, f1r, f2r, w1b, w2b,
    in_sem, w_sem, send_sem, r0_sem, r1_sem, rms_sem, rmr_sem, rqs_sem, rqr_sem, d2s_sem,
):
    nb, tok, dm = x_hbm.shape
    slots = xs.shape[1]
    n_slots = phi_hbm.shape[1]
    n_exp = slots // 16
    d = lax.axis_index("data")
    s = lax.axis_index("seq")
    xc, core = s // 2, s % 2
    to_p = {"data": d, "seq": 2 * xc + (1 - core)}
    to_x = {"data": d, "seq": 2 * (1 - xc) + core}
    to_y = {"data": 1 - d, "seq": s}

    def remote(src, dst, send, recv, dev):
        return pltpu.make_async_remote_copy(src_ref=src, dst_ref=dst, send_sem=send, recv_sem=recv, device_id=dev, device_id_type=pl.DeviceIdType.MESH)

    def weight_copies(e, slot):
        return (
            pltpu.make_async_copy(w1_hbm.at[n_exp * d + e], w1b.at[slot], w_sem.at[slot]),
            pltpu.make_async_copy(w2_hbm.at[n_exp * d + e], w2b.at[slot], w_sem.at[slot]),
        )

    barrier = pltpu.get_barrier_semaphore()
    for dev in (to_p, to_x, to_y):
        pl.semaphore_signal(barrier, inc=1, device_id=dev, device_id_type=pl.DeviceIdType.MESH)

    phi = ct.at[3, nb - 1, 0:dm]
    pnt = xs.at[2 * nb - 1]
    loads = [
        pltpu.make_async_copy(x_hbm, xg.at[0, :, 0], in_sem.at[0]),
        pltpu.make_async_copy(phi_hbm.at[:, pl.ds(pl.multiple_of(s * (n_slots // 4) + d * slots, slots), slots)], phi, in_sem.at[1]),
        pltpu.make_async_copy(len_hbm, len_ref, in_sem.at[2]),
        pltpu.make_async_copy(scale_hbm, scale_ref, in_sem.at[3]),
    ]
    for c in loads:
        c.start()

    by_x, by_y, by_p = send_sem.at[0], send_sem.at[1], send_sem.at[2]

    def blocks(ref, sem):
        return pltpu.make_async_copy(ref, ref, sem)

    def send_x(b):
        return remote(xg.at[0, b, 0], xg.at[1, b, 0], by_x, r0_sem.at[b], to_x)

    def send_y(b):
        return remote(xg.at[0, b, 0], xg.at[2, b, 0], by_y, r0_sem.at[b ^ 1], to_y)

    def send_p(b):
        return remote(xg.at[0, b, 0], xg.at[0, b, 1], by_p, r1_sem.at[b], to_p)

    cuts = (slice(0, tok // 2), slice(tok // 2, tok))

    def fwd_across(r, b, h, send, dev):
        part = cuts[h]
        return remote(xg.at[r, b, 0, part], xg.at[3, b, 0, part], send, r0_sem.at[4 + 2 * (b // 2) + h], dev)

    def arrive_pair(j):
        other = j + 1 - 2 * (j % 2)
        blocks(xg.at[0, 0], r0_sem.at[j]).wait()
        for r, b in ((1, j), (2, other)):
            remote(xg.at[r, b, 0], xg.at[r, b, 1], by_p, r1_sem.at[nb + j], to_p).start()

        @pl.when(j % 2 == 0)
        def _():
            for h in range(2):
                fwd_across(1, j, h, by_y, to_y).start()
                fwd_across(2, other, h, by_x, to_x).start()

    def arrive_across(j, h):
        part = cuts[h]
        blocks(xg.at[0, 0, :, part], r0_sem.at[4 + 2 * j + h]).wait()
        for b in (2 * j, 2 * j + 1):
            remote(xg.at[3, b, 0, part], xg.at[3, b, 1, part], by_p, r1_sem.at[2 * nb + j], to_p).start()

    rm_x = remote(rm.at[0, 0], rm.at[1, 0], rms_sem.at[0], rmr_sem.at[0], to_x)
    rm_y = remote(rm.at[0, 0], rm.at[2, 0], rms_sem.at[0], rmr_sem.at[0], to_y)
    rm_f = remote(rm.at[1, 0], rm.at[3, 0], rms_sem.at[0], rmr_sem.at[1], to_y)
    rm_p = [remote(rm.at[r, 0], rm.at[r, 1], rms_sem.at[1], rmr_sem.at[(2, 3, 3, 4)[r]], to_p) for r in range(4)]

    def phase_dispatch(acc, m_s, z_s):
        loads[2].wait()
        pos = s * tok + lax.broadcasted_iota(jnp.int32, (1, tok), 1)
        for b in range(nb):
            rm[0, 0, b:b + 1, :] = jnp.where(pos < len_ref[b], 0.0, NEG_FILL)
        loads[0].wait()
        pl.semaphore_wait(barrier, 3)
        rm_x.start()
        rm_y.start()
        rm_p[0].start()
        for b in range(nb):
            send_x(b).start()
            send_y(b ^ 1).start()
        for b in range(nb):
            send_p(b).start()
        for e in range(RING):
            for c in weight_copies(e, e):
                c.start()
        loads[3].wait()
        g2 = scale_ref[0] * LOG2E
        loads[1].wait()
        v = phi[...].astype(F32)
        pnt[...] = (v * lax.rsqrt(jnp.sum(v * v, axis=0, keepdims=True) + EPSILON)).T.astype(BF16)
        blocks(rm.at[0], rmr_sem.at[0]).wait()
        for c in (rm_f, rm_p[1], rm_p[2]):
            c.start()

        def unit(r, b, first, last):
            q = (r // 2) * nb + b
            a = b if r < 2 else b + 1 - 2 * (b % 2)
            xb = xg[r, b].reshape(2 * tok, dm)
            xn = unit_rows(xb.astype(F32))
            lt = lax.dot_general(pnt[...], xn, (((1,), (1,)), ((), ())), preferred_element_type=F32) * g2
            lm = lt + jnp.concatenate([rm[r, k, pl.ds(b, 1), :] for k in range(2)], axis=1)
            mx = jnp.broadcast_to(jnp.max(lm, axis=1, keepdims=True), (slots, 128))
            if not first:
                m_old = m_s[a]
                mx = jnp.maximum(mx, m_old)
            e = jnp.exp2(lm - jnp.concatenate([mx] * 4, axis=1))
            z = (e[:, 0:128] + e[:, 128:256]) + (e[:, 256:384] + e[:, 384:512])
            part = jnp.dot(e.astype(BF16), xb, preferred_element_type=F32)
            cmax = jnp.max(lt, axis=0, keepdims=True)
            c = jnp.exp2(lt - cmax)
            rqs[0, r, pl.ds(b, 1), :] = cmax
            rqs[0, r, pl.ds(nb + b, 1), :] = jnp.sum(c, axis=0, keepdims=True)
            ct[r, b] = c.astype(BF16)
            if not first:
                corr = jnp.exp2(m_old - mx)
                z = z + z_s[a] * corr
                part = part + acc[a] * jnp.concatenate([corr] * 3, axis=1)
            if last:
                inv = 1.0 / jnp.broadcast_to(jnp.sum(z, axis=1, keepdims=True), (slots, 128))
                xs[q] = (part * jnp.concatenate([inv] * 3, axis=1)).astype(BF16)
            else:
                m_s[a] = mx
                z_s[a] = z
                acc[a] = part

        blocks(rm.at[0, 0], rmr_sem.at[2]).wait()

        @pl.loop(0, nb)
        def _(b):
            blocks(xg.at[0, 0, 0], r1_sem.at[b]).wait()
            unit(0, b, True, False)

        arrive_pair(0)
        blocks(rm.at[0], rmr_sem.at[3]).wait()

        @pl.loop(0, nb)
        def _(j):
            blocks(xg.at[0, 0], r1_sem.at[nb + j]).wait()
            unit(1, j, False, True)

            @pl.when(j < nb - 1)
            def _():
                arrive_pair(j + 1)

            @pl.when(j == nb - 1)
            def _():
                blocks(rm.at[0, 0], rmr_sem.at[1]).wait()
                rm_p[3].start()
                arrive_across(0, 0)

            unit(2, j + 1 - 2 * (j % 2), True, False)

        arrive_across(0, 1)
        blocks(rm.at[0, 0], rmr_sem.at[4]).wait()

        blocks(xg.at[0, 0], r1_sem.at[2 * nb]).wait()

        @pl.loop(0, 2)
        def _(b):
            unit(3, b, False, True)
            for h in range(2):
                @pl.when(b == h)
                def _():
                    arrive_across(1, h)

        blocks(xg.at[0, 0], r1_sem.at[2 * nb + 1]).wait()

        @pl.loop(2, nb)
        def _(b):
            unit(3, b, False, True)

        blocks(xg.at[0, 0:3], by_x).wait()
        blocks(xg.at[0, 0:3], by_y).wait()
        blocks(xg.at[0:2], by_p).wait()
        blocks(rm.at[0:3, 0], rms_sem.at[0]).wait()
        blocks(rm.at[0:2], rms_sem.at[1]).wait()

    pl.run_scoped(
        phase_dispatch,
        pltpu.VMEM((nb, slots, dm), F32),
        pltpu.VMEM((nb, slots, 128), F32),
        pltpu.VMEM((nb, slots, 128), F32),
    )

    rq_copies = [remote(rqs.at[k], rqr.at[k], rqs_sem.at[0], rqr_sem.at[k], dev) for k, dev in enumerate((to_p, to_x, to_y))]

    def merge(k):
        rq_copies[k].wait()
        for r in range(4):
            if k == 0:
                theirs = jnp.concatenate([rqr[k, r][:, tok:], rqr[k, r][:, :tok]], axis=1)
            else:
                theirs = rqr[k, r ^ k]
            mine = rqs[k, r]
            top = jnp.maximum(mine[:nb], theirs[:nb])
            low = mine[nb:] * jnp.exp2(mine[:nb] - top) + theirs[nb:] * jnp.exp2(theirs[:nb] - top)
            rqs[k + 1, r, :nb] = top
            rqs[k + 1, r, nb:] = low
            if k == 2:
                wrow[r] = jnp.exp2(rqs[0, r][:nb] - top)
        if k < 2:
            rq_copies[k + 1].start()

    rq_copies[0].start()

    def ffn(es):
        for e in es:
            blocks(w1b.at[0:2], w_sem.at[e % RING]).wait()
        rows = [pl.ds(pl.multiple_of(e * 16, 16), 16) for e in es]
        xe = [xs[:, r, :].reshape(2 * nb * 16, dm) for r in rows]
        hs = [jnp.dot(x, w1b[e % RING], preferred_element_type=F32) for x, e in zip(xe, es)]
        ys = [jnp.dot(gelu_tanh(h).astype(BF16), w2b[e % RING], preferred_element_type=F32) for h, e in zip(hs, es)]
        for y, r in zip(ys, rows):
            xs[:, r, :] = y.astype(BF16).reshape(2 * nb, 16, dm)
        for e in es:
            @pl.when(e + RING < n_exp)
            def _():
                for c in weight_copies(e + RING, e % RING):
                    c.start()

    ffn([0, 1])

    @pl.loop(0, (n_exp - 8) // 4)
    def _(i):
        ffn([4 * i + 2 + k for k in range(4)])
        for k in range(3):
            @pl.when(i == 2 * k + 1)
            def _():
                merge(k)

    @pl.loop(0, 3)
    def _(i):
        ffn([n_exp - 6 + 2 * i, n_exp - 5 + 2 * i])

    def phase_combine(d2s, stash):
        def d2_start(r, b, g):
            remote(d2s.at[r, b], d2r.at[r, b], d2s_sem.at[g], r1_sem.at[g], to_p).start()

        def d2_wait(g, count):
            blocks(d2s.at[0, 0:count], d2s_sem.at[g]).wait()
            blocks(d2r.at[0, 0:count], r1_sem.at[g]).wait()

        def half_sum(r, b, cols):
            yt = xs[(r // 2) * nb + b].astype(F32).T.astype(BF16)
            return jnp.dot(yt, ct[r, b, :, cols], preferred_element_type=F32) * wrow[r, pl.ds(b, 1), :][:, cols]

        def comp(r, b, g):
            d2s[r, b] = half_sum(r, b, slice(tok, 2 * tok)).astype(BF16)
            d2_start(r, b, g)

        def mine(r, b):
            return half_sum(r, b, slice(0, tok))

        def h_start(b, odd):
            send, dev = (by_y, to_y) if odd else (by_x, to_x)
            remote(d2s.at[3, b], hr.at[b], send, r0_sem.at[b // 2], dev).start()

        def f1_start(b):
            remote(d2s.at[1, b], f1r.at[b], by_x, r0_sem.at[nb + b], to_x).start()

        def f2_start(b):
            remote(d2s.at[2, b], f2r.at[b], by_y, r0_sem.at[nb + b], to_y).start()

        @pl.loop(0, 2)
        def _(b):
            comp(3, b, b)

        @pl.loop(0, 2)
        def _(b):
            stash[b] = mine(3, b)

        for b in (0, 1):
            d2_wait(b, 1)
            d2s[3, b] = (stash[b] + d2r[3, b].astype(F32)).astype(BF16)
            h_start(b, b == 1)

        @pl.loop(2, 4)
        def _(b):
            comp(3, b, 7)

        @pl.loop(2, 4)
        def _(b):
            stash[b] = mine(3, b)

        comp(1, 0, 2)
        comp(2, 1, 2)
        d2_wait(7, 2)
        for b in (2, 3):
            d2s[3, b] = (stash[b] + d2r[3, b].astype(F32)).astype(BF16)
            h_start(b, b == 3)
        comp(1, 2, 3)
        comp(2, 3, 3)

        @pl.loop(0, nb // 2)
        def _(j):
            b0, b1 = 2 * j, 2 * j + 1
            d2_wait(2 + j, 2)
            d2s[1, b0] = (mine(1, b0) + d2r[1, b0].astype(F32)).astype(BF16)
            f1_start(b0)
            d2s[2, b1] = (mine(2, b1) + d2r[2, b1].astype(F32)).astype(BF16)
            f2_start(b1)
            comp(1, b1, 4 + j)
            comp(2, b0, 4 + j)

        @pl.loop(0, nb // 2)
        def _(j):
            b0, b1 = 2 * j, 2 * j + 1
            t1, t2 = mine(1, b1), mine(2, b0)
            d2_wait(4 + j, 2)
            t1 += d2r[1, b1].astype(F32)
            t2 += d2r[2, b0].astype(F32)
            blocks(hr.at[0:2], r0_sem.at[j]).wait()
            d2s[1, b1] = (t1 + hr[b1].astype(F32)).astype(BF16)
            f1_start(b1)
            d2s[2, b0] = (t2 + hr[b0].astype(F32)).astype(BF16)
            f2_start(b0)

        @pl.loop(0, nb)
        def _(b):
            comp(0, b, 6)

        @pl.loop(0, nb)
        def _(b):
            stash[b] = mine(0, b)

        d2_wait(6, nb)

        @pl.loop(0, nb)
        def _(b):
            base = stash[b] + d2r[0, b].astype(F32)
            blocks(f1r.at[0:2], r0_sem.at[nb + b]).wait()
            pos = s * tok + lax.broadcasted_iota(jnp.int32, (1, tok), 1)
            y = (base + f1r[b].astype(F32) + f2r[b].astype(F32)) / rqs[3, 0, pl.ds(nb + b, 1), :tok]
            y = jnp.where(pos < len_ref[b], y, 0.0)
            out_ref[b] = y.T.astype(BF16)

        blocks(xg.at[0, 0:3], by_x).wait()
        blocks(xg.at[0, 0:3], by_y).wait()

    pl.run_scoped(
        phase_combine,
        pltpu.VMEM((4, nb, dm, tok), BF16),
        pltpu.VMEM((nb, dm, tok), F32),
    )


def solution(mesh):
    def local_layer(tok_blk, len_blk, slot_param, logit_scale, w_in, w_out):
        nb, tok, dm = tok_blk.shape
        n_slots = slot_param.shape[1]
        slots = n_slots // 8
        ff = w_in.shape[2]
        hbm = pl.BlockSpec(memory_space=pl.ANY)
        dma = pltpu.SemaphoreType.DMA
        return pl.pallas_call(
            layer_kernel,
            out_shape=pltpu.VMEM((nb, tok, dm), BF16),
            in_specs=[hbm] * 6,
            out_specs=pl.BlockSpec(memory_space=pltpu.VMEM),
            scratch_shapes=[
                pltpu.SMEM((1,), F32),
                pltpu.SMEM((nb,), jnp.int32),
                pltpu.VMEM((4, nb, 2, tok, dm), BF16),
                pltpu.VMEM((4, 2, nb, tok), F32),
                pltpu.VMEM((4, 4, 2 * nb, 2 * tok), F32),
                pltpu.VMEM((3, 4, 2 * nb, 2 * tok), F32),
                pltpu.VMEM((4, nb, 2 * tok), F32),
                pltpu.VMEM((4, nb, slots, 2 * tok), BF16),
                pltpu.VMEM((2 * nb, slots, dm), BF16),
                pltpu.VMEM((4, nb, dm, tok), BF16),
                pltpu.VMEM((nb, dm, tok), BF16),
                pltpu.VMEM((nb, dm, tok), BF16),
                pltpu.VMEM((nb, dm, tok), BF16),
                pltpu.VMEM((RING, dm, ff), BF16),
                pltpu.VMEM((RING, ff, dm), BF16),
                dma((4,)), dma((RING,)), dma((3,)), dma((2 * nb,)), dma((2 * nb + 2,)), dma((2,)), dma((5,)), dma((1,)), dma((3,)), dma((8,)),
            ],
            compiler_params=pltpu.CompilerParams(collective_id=0, has_side_effects=True, vmem_limit_bytes=66_250_000),
            name="soft_moe_layer",
        )(logit_scale.reshape(1), len_blk, tok_blk, slot_param, w_in, w_out)

    return jax.shard_map(local_layer, mesh=mesh, in_specs=(P("data", "seq", None), P("data"), P(None, None), P(), P("seq", None, None), P("seq", None, None)), out_specs=P("data", "seq", None), check_vma=False)
```

```python
import functools
import math

import jax
import jax.numpy as jnp
from jax import lax
from jax.experimental import pallas as pl
from jax.experimental.pallas import tpu as pltpu
from jax.sharding import PartitionSpec as P

EPSILON = 1e-6
NEG_FILL = -1e30
LOG2E = 1.0 / math.log(2.0)
F32 = jnp.float32
BF16 = jnp.bfloat16
RING = 14


def unit_rows(v32):
    return (v32 * lax.rsqrt(jnp.sum(v32 * v32, axis=1, keepdims=True) + EPSILON)).astype(BF16)


def gelu_tanh(h):
    inner = h * (math.sqrt(2.0 / math.pi) + (math.sqrt(2.0 / math.pi) * 0.044715) * (h * h))
    half = 0.5 * h
    return half + half * jnp.tanh(inner)


def row_of(col, rows):
    return jnp.broadcast_to(col, (rows, 128)).T[0:1, :]


def layer_kernel(
    scale_hbm, len_hbm, x_hbm, phi_hbm, w1_hbm, w2_hbm, out_ref,
    scale_ref, len_ref, xg, rm, rqs, rqr, wrow, ct, xs, d2r, hr, f1r, f2r, w1b, w2b,
    in_sem, w_sem, send_sem, r0_sem, r1_sem, rms_sem, rmr_sem, rqs_sem, rqr_sem, d2s_sem,
):
    nb, tok, dm = x_hbm.shape
    slots = xs.shape[1]
    n_slots = phi_hbm.shape[1]
    n_exp = slots // 16
    d = lax.axis_index("data")
    s = lax.axis_index("seq")
    xc, core = s // 2, s % 2
    to_p = {"data": d, "seq": 2 * xc + (1 - core)}
    to_x = {"data": d, "seq": 2 * (1 - xc) + core}
    to_y = {"data": 1 - d, "seq": s}

    def remote(src, dst, send, recv, dev):
        return pltpu.make_async_remote_copy(src_ref=src, dst_ref=dst, send_sem=send, recv_sem=recv, device_id=dev, device_id_type=pl.DeviceIdType.MESH)

    def weight_copies(e, slot):
        return (
            pltpu.make_async_copy(w1_hbm.at[n_exp * d + e], w1b.at[slot], w_sem.at[slot]),
            pltpu.make_async_copy(w2_hbm.at[n_exp * d + e], w2b.at[slot], w_sem.at[slot]),
        )

    barrier = pltpu.get_barrier_semaphore()
    for dev in (to_p, to_x, to_y):
        pl.semaphore_signal(barrier, inc=1, device_id=dev, device_id_type=pl.DeviceIdType.MESH)

    phi = ct.at[3, nb - 1, 0:dm]
    pnt = xs.at[2 * nb - 1]
    loads = [
        pltpu.make_async_copy(x_hbm, xg.at[0, :, 0], in_sem.at[0]),
        pltpu.make_async_copy(phi_hbm.at[:, pl.ds(pl.multiple_of(s * (n_slots // 4) + d * slots, slots), slots)], phi, in_sem.at[1]),
        pltpu.make_async_copy(len_hbm, len_ref, in_sem.at[2]),
        pltpu.make_async_copy(scale_hbm, scale_ref, in_sem.at[3]),
    ]
    for c in loads:
        c.start()

    by_x, by_y, by_p = send_sem.at[0], send_sem.at[1], send_sem.at[2]

    def blocks(ref, sem):
        return pltpu.make_async_copy(ref, ref, sem)

    def send_x(b):
        return remote(xg.at[0, b, 0], xg.at[1, b, 0], by_x, r0_sem.at[b], to_x)

    def send_y(b):
        return remote(xg.at[0, b, 0], xg.at[2, b, 0], by_y, r0_sem.at[b], to_y)

    def send_p(b):
        return remote(xg.at[0, b, 0], xg.at[0, b, 1], by_p, r1_sem.at[b], to_p)

    def fwd_across(r, b, part, send, dev):
        remote(xg.at[r, b, 0, part], xg.at[3, b, 0, part], send, r0_sem.at[nb + b], dev).start()

    def arrive_pair(b):
        blocks(xg.at[0, 0], r0_sem.at[b]).wait()
        for r in (1, 2):
            remote(xg.at[r, b, 0], xg.at[r, b, 1], by_p, r1_sem.at[nb + b], to_p).start()
        fwd_across(1, b, slice(0, tok // 2), by_y, to_y)
        fwd_across(2, b, slice(tok // 2, tok), by_x, to_x)

    def arrive_across(b):
        blocks(xg.at[0, 0, 0], r0_sem.at[nb + b]).wait()
        remote(xg.at[3, b, 0], xg.at[3, b, 1], by_p, r1_sem.at[2 * nb + b], to_p).start()

    rm_x = remote(rm.at[0, 0], rm.at[1, 0], rms_sem.at[0], rmr_sem.at[0], to_x)
    rm_y = remote(rm.at[0, 0], rm.at[2, 0], rms_sem.at[0], rmr_sem.at[0], to_y)
    rm_f = remote(rm.at[1, 0], rm.at[3, 0], rms_sem.at[0], rmr_sem.at[1], to_y)
    rm_p = [remote(rm.at[r, 0], rm.at[r, 1], rms_sem.at[1], rmr_sem.at[(2, 3, 3, 4)[r]], to_p) for r in range(4)]

    def phase_dispatch(acc, m_s, z_s):
        loads[2].wait()
        pos = s * tok + lax.broadcasted_iota(jnp.int32, (1, tok), 1)
        for b in range(nb):
            rm[0, 0, b:b + 1, :] = jnp.where(pos < len_ref[b], 0.0, NEG_FILL)
        loads[0].wait()
        pl.semaphore_wait(barrier, 3)
        rm_x.start()
        rm_y.start()
        rm_p[0].start()
        for b in range(nb):
            send_x(b).start()
            send_y(b).start()
        for b in range(nb):
            send_p(b).start()
        for e in range(RING):
            for c in weight_copies(e, e):
                c.start()
        loads[3].wait()
        g2 = scale_ref[0] * LOG2E
        loads[1].wait()
        v = phi[...].astype(F32)
        pnt[...] = (v * lax.rsqrt(jnp.sum(v * v, axis=0, keepdims=True) + EPSILON)).T.astype(BF16)
        blocks(rm.at[0], rmr_sem.at[0]).wait()
        for c in (rm_f, rm_p[1], rm_p[2]):
            c.start()

        def unit(r, b, first, last):
            q = (r // 2) * nb + b
            a = b
            xb = xg[r, b].reshape(2 * tok, dm)
            xn = unit_rows(xb.astype(F32))
            lt = lax.dot_general(pnt[...], xn, (((1,), (1,)), ((), ())), preferred_element_type=F32) * g2
            lm = lt + jnp.concatenate([rm[r, k, pl.ds(b, 1), :] for k in range(2)], axis=1)
            mx = jnp.broadcast_to(jnp.max(lm, axis=1, keepdims=True), (slots, 128))
            if not first:
                m_old = m_s[a]
                mx = jnp.maximum(mx, m_old)
            e = jnp.exp2(lm - jnp.concatenate([mx] * 4, axis=1))
            z = (e[:, 0:128] + e[:, 128:256]) + (e[:, 256:384] + e[:, 384:512])
            part = jnp.dot(e.astype(BF16), xb, preferred_element_type=F32)
            cmax = jnp.max(lt, axis=0, keepdims=True)
            c = jnp.exp2(lt - cmax)
            rqs[0, r, pl.ds(b, 1), :] = cmax
            rqs[0, r, pl.ds(nb + b, 1), :] = jnp.sum(c, axis=0, keepdims=True)
            ct[r, b] = c.astype(BF16)
            if not first:
                corr = jnp.exp2(m_old - mx)
                z = z + z_s[a] * corr
                part = part + acc[a] * jnp.concatenate([corr] * 3, axis=1)
            if last:
                inv = 1.0 / jnp.broadcast_to(jnp.sum(z, axis=1, keepdims=True), (slots, 128))
                xs[q] = (part * jnp.concatenate([inv] * 3, axis=1)).astype(BF16)
            else:
                m_s[a] = mx
                z_s[a] = z
                acc[a] = part

        blocks(rm.at[0, 0], rmr_sem.at[2]).wait()

        @pl.loop(0, nb)
        def _(b):
            blocks(xg.at[0, 0, 0], r1_sem.at[b]).wait()
            unit(0, b, True, False)

        arrive_pair(0)
        blocks(rm.at[0], rmr_sem.at[3]).wait()

        @pl.loop(0, nb)
        def _(j):
            blocks(xg.at[0, 0], r1_sem.at[nb + j]).wait()
            unit(1, j, False, True)

            @pl.when(j < nb - 1)
            def _():
                arrive_pair(j + 1)

            @pl.when(j == nb - 1)
            def _():
                blocks(rm.at[0, 0], rmr_sem.at[1]).wait()
                rm_p[3].start()
                arrive_across(0)

            unit(2, j, True, False)

        arrive_across(1)
        blocks(rm.at[0, 0], rmr_sem.at[4]).wait()

        @pl.loop(0, nb)
        def _(b):
            @pl.when(b == nb - 2)
            def _():
                arrive_across(nb - 2)
                arrive_across(nb - 1)

            blocks(xg.at[0, 0, 0], r1_sem.at[2 * nb + b]).wait()
            unit(3, b, False, True)

        blocks(xg.at[0, 0:3], by_x).wait()
        blocks(xg.at[0, 0:3], by_y).wait()
        blocks(xg.at[0:2], by_p).wait()
        blocks(rm.at[0:3, 0], rms_sem.at[0]).wait()
        blocks(rm.at[0:2], rms_sem.at[1]).wait()

    pl.run_scoped(
        phase_dispatch,
        pltpu.VMEM((nb, slots, dm), F32),
        pltpu.VMEM((nb, slots, 128), F32),
        pltpu.VMEM((nb, slots, 128), F32),
    )

    rq_copies = [remote(rqs.at[k], rqr.at[k], rqs_sem.at[0], rqr_sem.at[k], dev) for k, dev in enumerate((to_p, to_x, to_y))]

    def merge(k):
        rq_copies[k].wait()
        for r in range(4):
            if k == 0:
                theirs = jnp.concatenate([rqr[k, r][:, tok:], rqr[k, r][:, :tok]], axis=1)
            else:
                theirs = rqr[k, r ^ k]
            mine = rqs[k, r]
            top = jnp.maximum(mine[:nb], theirs[:nb])
            low = mine[nb:] * jnp.exp2(mine[:nb] - top) + theirs[nb:] * jnp.exp2(theirs[:nb] - top)
            rqs[k + 1, r, :nb] = top
            rqs[k + 1, r, nb:] = low
            if k == 2:
                wrow[r] = jnp.exp2(rqs[0, r][:nb] - top)
        if k < 2:
            rq_copies[k + 1].start()

    rq_copies[0].start()

    def ffn(es):
        for e in es:
            blocks(w1b.at[0:2], w_sem.at[e % RING]).wait()
        rows = [pl.ds(pl.multiple_of(e * 16, 16), 16) for e in es]
        xe = [xs[:, r, :].reshape(2 * nb * 16, dm) for r in rows]
        hs = [jnp.dot(x, w1b[e % RING], preferred_element_type=F32) for x, e in zip(xe, es)]
        ys = [jnp.dot(gelu_tanh(h).astype(BF16), w2b[e % RING], preferred_element_type=F32) for h, e in zip(hs, es)]
        for y, r in zip(ys, rows):
            xs[:, r, :] = y.astype(BF16).reshape(2 * nb, 16, dm)
        for e in es:
            @pl.when(e + RING < n_exp)
            def _():
                for c in weight_copies(e + RING, e % RING):
                    c.start()

    ffn([0, 1])

    @pl.loop(0, (n_exp - 8) // 4)
    def _(i):
        ffn([4 * i + 2 + k for k in range(4)])
        for k in range(3):
            @pl.when(i == 2 * k + 1)
            def _():
                merge(k)

    @pl.loop(0, 3)
    def _(i):
        ffn([n_exp - 6 + 2 * i, n_exp - 5 + 2 * i])

    def phase_combine(d2s, stash):
        def d2_start(r, b, g):
            remote(d2s.at[r, b], d2r.at[r, b], d2s_sem.at[g], r1_sem.at[g], to_p).start()

        def d2_wait(g, count):
            blocks(d2s.at[0, 0:count], d2s_sem.at[g]).wait()
            blocks(d2r.at[0, 0:count], r1_sem.at[g]).wait()

        def half_sum(r, b, cols):
            yt = xs[(r // 2) * nb + b].astype(F32).T.astype(BF16)
            return jnp.dot(yt, ct[r, b, :, cols], preferred_element_type=F32) * wrow[r, pl.ds(b, 1), :][:, cols]

        def comp(r, b, g):
            d2s[r, b] = half_sum(r, b, slice(tok, 2 * tok)).astype(BF16)
            d2_start(r, b, g)

        def mine(r, b):
            return half_sum(r, b, slice(0, tok))

        def h_start(b, odd):
            send, dev = (by_y, to_y) if odd else (by_x, to_x)
            remote(d2s.at[3, b], hr.at[b], send, r0_sem.at[b // 2], dev).start()

        def f1_start(b):
            remote(d2s.at[1, b], f1r.at[b], by_x, r0_sem.at[nb + b], to_x).start()

        def f2_start(b):
            remote(d2s.at[2, b], f2r.at[b], by_y, r0_sem.at[nb + b], to_y).start()

        @pl.loop(0, 2)
        def _(b):
            comp(3, b, b)

        @pl.loop(0, 2)
        def _(b):
            stash[b] = mine(3, b)

        for b in (0, 1):
            d2_wait(b, 1)
            d2s[3, b] = (stash[b] + d2r[3, b].astype(F32)).astype(BF16)
            h_start(b, b == 1)

        @pl.loop(2, 4)
        def _(b):
            comp(3, b, 7)

        @pl.loop(2, 4)
        def _(b):
            stash[b] = mine(3, b)

        comp(1, 0, 2)
        comp(2, 1, 2)
        d2_wait(7, 2)
        for b in (2, 3):
            d2s[3, b] = (stash[b] + d2r[3, b].astype(F32)).astype(BF16)
            h_start(b, b == 3)
        comp(1, 2, 3)
        comp(2, 3, 3)

        @pl.loop(0, nb // 2)
        def _(j):
            b0, b1 = 2 * j, 2 * j + 1
            d2_wait(2 + j, 2)
            d2s[1, b0] = (mine(1, b0) + d2r[1, b0].astype(F32)).astype(BF16)
            f1_start(b0)
            d2s[2, b1] = (mine(2, b1) + d2r[2, b1].astype(F32)).astype(BF16)
            f2_start(b1)
            comp(1, b1, 4 + j)
            comp(2, b0, 4 + j)

        @pl.loop(0, nb // 2)
        def _(j):
            b0, b1 = 2 * j, 2 * j + 1
            t1, t2 = mine(1, b1), mine(2, b0)
            d2_wait(4 + j, 2)
            t1 += d2r[1, b1].astype(F32)
            t2 += d2r[2, b0].astype(F32)
            blocks(hr.at[0:2], r0_sem.at[j]).wait()
            d2s[1, b1] = (t1 + hr[b1].astype(F32)).astype(BF16)
            f1_start(b1)
            d2s[2, b0] = (t2 + hr[b0].astype(F32)).astype(BF16)
            f2_start(b0)

        @pl.loop(0, nb)
        def _(b):
            comp(0, b, 6)

        @pl.loop(0, nb)
        def _(b):
            stash[b] = mine(0, b)

        d2_wait(6, nb)

        @pl.loop(0, nb)
        def _(b):
            base = stash[b] + d2r[0, b].astype(F32)
            blocks(f1r.at[0:2], r0_sem.at[nb + b]).wait()
            pos = s * tok + lax.broadcasted_iota(jnp.int32, (1, tok), 1)
            y = (base + f1r[b].astype(F32) + f2r[b].astype(F32)) / rqs[3, 0, pl.ds(nb + b, 1), :tok]
            y = jnp.where(pos < len_ref[b], y, 0.0)
            out_ref[b] = y.T.astype(BF16)

        blocks(xg.at[0, 0:3], by_x).wait()
        blocks(xg.at[0, 0:3], by_y).wait()

    pl.run_scoped(
        phase_combine,
        pltpu.VMEM((4, nb, dm, tok), BF16),
        pltpu.VMEM((nb, dm, tok), F32),
    )


def solution(mesh):
    def local_layer(tok_blk, len_blk, slot_param, logit_scale, w_in, w_out):
        nb, tok, dm = tok_blk.shape
        n_slots = slot_param.shape[1]
        slots = n_slots // 8
        ff = w_in.shape[2]
        hbm = pl.BlockSpec(memory_space=pl.ANY)
        dma = pltpu.SemaphoreType.DMA
        return pl.pallas_call(
            layer_kernel,
            out_shape=pltpu.VMEM((nb, tok, dm), BF16),
            in_specs=[hbm] * 6,
            out_specs=pl.BlockSpec(memory_space=pltpu.VMEM),
            scratch_shapes=[
                pltpu.SMEM((1,), F32),
                pltpu.SMEM((nb,), jnp.int32),
                pltpu.VMEM((4, nb, 2, tok, dm), BF16),
                pltpu.VMEM((4, 2, nb, tok), F32),
                pltpu.VMEM((4, 4, 2 * nb, 2 * tok), F32),
                pltpu.VMEM((3, 4, 2 * nb, 2 * tok), F32),
                pltpu.VMEM((4, nb, 2 * tok), F32),
                pltpu.VMEM((4, nb, slots, 2 * tok), BF16),
                pltpu.VMEM((2 * nb, slots, dm), BF16),
                pltpu.VMEM((4, nb, dm, tok), BF16),
                pltpu.VMEM((nb, dm, tok), BF16),
                pltpu.VMEM((nb, dm, tok), BF16),
                pltpu.VMEM((nb, dm, tok), BF16),
                pltpu.VMEM((RING, dm, ff), BF16),
                pltpu.VMEM((RING, ff, dm), BF16),
                dma((4,)), dma((RING,)), dma((3,)), dma((2 * nb,)), dma((3 * nb,)), dma((2,)), dma((5,)), dma((1,)), dma((3,)), dma((8,)),
            ],
            compiler_params=pltpu.CompilerParams(collective_id=0, has_side_effects=True, vmem_limit_bytes=66_250_000),
            name="soft_moe_layer",
        )(logit_scale.reshape(1), len_blk, tok_blk, slot_param, w_in, w_out)

    return jax.shard_map(local_layer, mesh=mesh, in_specs=(P("data", "seq", None), P("data"), P(None, None), P(), P("seq", None, None), P("seq", None, None)), out_specs=P("data", "seq", None), check_vma=False)
```

```python
import functools
import math

import jax
import jax.numpy as jnp
from jax import lax
from jax.experimental import pallas as pl
from jax.experimental.pallas import tpu as pltpu
from jax.sharding import PartitionSpec as P

EPSILON = 1e-6
NEG_FILL = -1e30
LOG2E = 1.0 / math.log(2.0)
F32 = jnp.float32
BF16 = jnp.bfloat16
RING = 14


def unit_rows(v32):
    return (v32 * lax.rsqrt(jnp.sum(v32 * v32, axis=1, keepdims=True) + EPSILON)).astype(BF16)


def gelu_tanh(h):
    inner = h * (math.sqrt(2.0 / math.pi) + (math.sqrt(2.0 / math.pi) * 0.044715) * (h * h))
    half = 0.5 * h
    return half + half * jnp.tanh(inner)


def row_of(col, rows):
    return jnp.broadcast_to(col, (rows, 128)).T[0:1, :]


def layer_kernel(
    scale_hbm, len_hbm, x_hbm, phi_hbm, w1_hbm, w2_hbm, out_ref,
    scale_ref, len_ref, xg, rm, rqs, rqr, wrow, ct, xs, d2r, hr, f1r, f2r, w1b, w2b,
    in_sem, w_sem, send_sem, r0_sem, r1_sem, rms_sem, rmr_sem, rqs_sem, rqr_sem, d2s_sem,
):
    nb, tok, dm = x_hbm.shape
    slots = xs.shape[1]
    n_slots = phi_hbm.shape[1]
    n_exp = slots // 16
    d = lax.axis_index("data")
    s = lax.axis_index("seq")
    xc, core = s // 2, s % 2
    to_p = {"data": d, "seq": 2 * xc + (1 - core)}
    to_x = {"data": d, "seq": 2 * (1 - xc) + core}
    to_y = {"data": 1 - d, "seq": s}

    def remote(src, dst, send, recv, dev):
        return pltpu.make_async_remote_copy(src_ref=src, dst_ref=dst, send_sem=send, recv_sem=recv, device_id=dev, device_id_type=pl.DeviceIdType.MESH)

    def weight_copies(e, slot):
        return (
            pltpu.make_async_copy(w1_hbm.at[n_exp * d + e], w1b.at[slot], w_sem.at[slot]),
            pltpu.make_async_copy(w2_hbm.at[n_exp * d + e], w2b.at[slot], w_sem.at[slot]),
        )

    barrier = pltpu.get_barrier_semaphore()
    for dev in (to_p, to_x, to_y):
        pl.semaphore_signal(barrier, inc=1, device_id=dev, device_id_type=pl.DeviceIdType.MESH)

    phi = ct.at[3, nb - 1, 0:dm]
    pnt = xs.at[2 * nb - 1]
    loads = [
        pltpu.make_async_copy(x_hbm, xg.at[0, :, 0], in_sem.at[0]),
        pltpu.make_async_copy(phi_hbm.at[:, pl.ds(pl.multiple_of(s * (n_slots // 4) + d * slots, slots), slots)], phi, in_sem.at[1]),
        pltpu.make_async_copy(len_hbm, len_ref, in_sem.at[2]),
        pltpu.make_async_copy(scale_hbm, scale_ref, in_sem.at[3]),
    ]
    for c in loads:
        c.start()

    by_x, by_y, by_p = send_sem.at[0], send_sem.at[1], send_sem.at[2]

    def blocks(ref, sem):
        return pltpu.make_async_copy(ref, ref, sem)

    def send_x(b):
        return remote(xg.at[0, b, 0], xg.at[1, b, 0], by_x, r0_sem.at[b], to_x)

    def send_y(b):
        return remote(xg.at[0, b, 0], xg.at[2, b, 0], by_y, r0_sem.at[b], to_y)

    def send_p(b):
        return remote(xg.at[0, b, 0], xg.at[0, b, 1], by_p, r1_sem.at[b], to_p)

    def fwd_across(r, b, part, send, dev):
        remote(xg.at[r, b, 0, part], xg.at[3, b, 0, part], send, r0_sem.at[nb + b], dev).start()

    def arrive_pair(b):
        blocks(xg.at[0, 0], r0_sem.at[b]).wait()
        for r in (1, 2):
            remote(xg.at[r, b, 0], xg.at[r, b, 1], by_p, r1_sem.at[nb + b], to_p).start()
        fwd_across(1, b, slice(0, tok // 2), by_y, to_y)
        fwd_across(2, b, slice(tok // 2, tok), by_x, to_x)

    def arrive_across(b):
        blocks(xg.at[0, 0, 0], r0_sem.at[nb + b]).wait()
        remote(xg.at[3, b, 0], xg.at[3, b, 1], by_p, r1_sem.at[2 * nb + b], to_p).start()

    rm_x = remote(rm.at[0, 0], rm.at[1, 0], rms_sem.at[0], rmr_sem.at[0], to_x)
    rm_y = remote(rm.at[0, 0], rm.at[2, 0], rms_sem.at[0], rmr_sem.at[0], to_y)
    rm_f = remote(rm.at[1, 0], rm.at[3, 0], rms_sem.at[0], rmr_sem.at[1], to_y)
    rm_p = [remote(rm.at[r, 0], rm.at[r, 1], rms_sem.at[1], rmr_sem.at[(2, 3, 3, 4)[r]], to_p) for r in range(4)]

    def phase_dispatch(acc, m_s, z_s):
        loads[2].wait()
        pos = s * tok + lax.broadcasted_iota(jnp.int32, (1, tok), 1)
        for b in range(nb):
            rm[0, 0, b:b + 1, :] = jnp.where(pos < len_ref[b], 0.0, NEG_FILL)
        loads[0].wait()
        pl.semaphore_wait(barrier, 3)
        rm_x.start()
        rm_y.start()
        rm_p[0].start()
        for b in range(nb):
            send_x(b).start()
            send_y(b).start()
        for b in range(nb):
            send_p(b).start()
        for e in range(RING):
            for c in weight_copies(e, e):
                c.start()
        loads[3].wait()
        g2 = scale_ref[0] * LOG2E
        loads[1].wait()
        v = phi[...].astype(F32)
        pnt[...] = (v * lax.rsqrt(jnp.sum(v * v, axis=0, keepdims=True) + EPSILON)).T.astype(BF16)
        blocks(rm.at[0], rmr_sem.at[0]).wait()
        for c in (rm_f, rm_p[1], rm_p[2]):
            c.start()

        def unit(r, b, first, last):
            q = (r // 2) * nb + b
            a = b
            xb = xg[r, b].reshape(2 * tok, dm)
            xn = unit_rows(xb.astype(F32))
            lt = lax.dot_general(pnt[...], xn, (((1,), (1,)), ((), ())), preferred_element_type=F32) * g2
            lm = lt + jnp.concatenate([rm[r, k, pl.ds(b, 1), :] for k in range(2)], axis=1)
            mx = jnp.broadcast_to(jnp.max(lm, axis=1, keepdims=True), (slots, 128))
            if not first:
                m_old = m_s[a]
                mx = jnp.maximum(mx, m_old)
            e = jnp.exp2(lm - jnp.concatenate([mx] * 4, axis=1))
            z = (e[:, 0:128] + e[:, 128:256]) + (e[:, 256:384] + e[:, 384:512])
            part = jnp.dot(e.astype(BF16), xb, preferred_element_type=F32)
            cmax = jnp.max(lt, axis=0, keepdims=True)
            c = jnp.exp2(lt - cmax)
            rqs[0, r, pl.ds(b, 1), :] = cmax
            rqs[0, r, pl.ds(nb + b, 1), :] = jnp.sum(c, axis=0, keepdims=True)
            ct[r, b] = c.astype(BF16)
            if not first:
                corr = jnp.exp2(m_old - mx)
                z = z + z_s[a] * corr
                part = part + acc[a] * jnp.concatenate([corr] * 3, axis=1)
            if last:
                inv = 1.0 / jnp.broadcast_to(jnp.sum(z, axis=1, keepdims=True), (slots, 128))
                xs[q] = (part * jnp.concatenate([inv] * 3, axis=1)).astype(BF16)
            else:
                m_s[a] = mx
                z_s[a] = z
                acc[a] = part

        blocks(rm.at[0, 0], rmr_sem.at[2]).wait()

        @pl.loop(0, nb)
        def _(b):
            blocks(xg.at[0, 0, 0], r1_sem.at[b]).wait()
            unit(0, b, True, False)

        arrive_pair(0)
        blocks(rm.at[0], rmr_sem.at[3]).wait()

        @pl.loop(0, nb)
        def _(j):
            blocks(xg.at[0, 0], r1_sem.at[nb + j]).wait()
            unit(1, j, False, True)

            @pl.when(j < nb - 1)
            def _():
                arrive_pair(j + 1)

            @pl.when(j == nb - 1)
            def _():
                blocks(rm.at[0, 0], rmr_sem.at[1]).wait()
                rm_p[3].start()
                arrive_across(0)

            unit(2, j, True, False)

        arrive_across(1)
        blocks(rm.at[0, 0], rmr_sem.at[4]).wait()

        @pl.loop(0, nb)
        def _(b):
            @pl.when(b == nb - 2)
            def _():
                arrive_across(nb - 2)
                arrive_across(nb - 1)

            blocks(xg.at[0, 0, 0], r1_sem.at[2 * nb + b]).wait()
            unit(3, b, False, True)

        blocks(xg.at[0, 0:3], by_x).wait()
        blocks(xg.at[0, 0:3], by_y).wait()
        blocks(xg.at[0:2], by_p).wait()
        blocks(rm.at[0:3, 0], rms_sem.at[0]).wait()
        blocks(rm.at[0:2], rms_sem.at[1]).wait()

    pl.run_scoped(
        phase_dispatch,
        pltpu.VMEM((nb, slots, dm), F32),
        pltpu.VMEM((nb, slots, 128), F32),
        pltpu.VMEM((nb, slots, 128), F32),
    )

    rq_copies = [remote(rqs.at[k], rqr.at[k], rqs_sem.at[0], rqr_sem.at[k], dev) for k, dev in enumerate((to_p, to_x, to_y))]

    def merge(k):
        rq_copies[k].wait()
        for r in range(4):
            if k == 0:
                theirs = jnp.concatenate([rqr[k, r][:, tok:], rqr[k, r][:, :tok]], axis=1)
            else:
                theirs = rqr[k, r ^ k]
            mine = rqs[k, r]
            top = jnp.maximum(mine[:nb], theirs[:nb])
            low = mine[nb:] * jnp.exp2(mine[:nb] - top) + theirs[nb:] * jnp.exp2(theirs[:nb] - top)
            rqs[k + 1, r, :nb] = top
            rqs[k + 1, r, nb:] = low
            if k == 2:
                wrow[r] = jnp.exp2(rqs[0, r][:nb] - top)
        if k < 2:
            rq_copies[k + 1].start()

    rq_copies[0].start()

    def ffn(es):
        for e in es:
            blocks(w1b.at[0:2], w_sem.at[e % RING]).wait()
        rows = [pl.ds(pl.multiple_of(e * 16, 16), 16) for e in es]
        xe = [xs[:, r, :].reshape(2 * nb * 16, dm) for r in rows]
        hs = [jnp.dot(x, w1b[e % RING], preferred_element_type=F32) for x, e in zip(xe, es)]
        ys = [jnp.dot(gelu_tanh(h).astype(BF16), w2b[e % RING], preferred_element_type=F32) for h, e in zip(hs, es)]
        for y, r in zip(ys, rows):
            xs[:, r, :] = y.astype(BF16).reshape(2 * nb, 16, dm)
        for e in es:
            @pl.when(e + RING < n_exp)
            def _():
                for c in weight_copies(e + RING, e % RING):
                    c.start()

    ffn([0, 1])

    @pl.loop(0, (n_exp - 8) // 4)
    def _(i):
        ffn([4 * i + 2 + k for k in range(4)])
        for k in range(3):
            @pl.when(i == 2 * k + 1)
            def _():
                merge(k)

    @pl.loop(0, 3)
    def _(i):
        ffn([n_exp - 6 + 2 * i, n_exp - 5 + 2 * i])

    def phase_combine(d2s, stash):
        def d2_start(r, b, g):
            remote(d2s.at[r, b], d2r.at[r, b], d2s_sem.at[g], r1_sem.at[g], to_p).start()

        def d2_wait(g, count):
            blocks(d2s.at[0, 0:count], d2s_sem.at[g]).wait()
            blocks(d2r.at[0, 0:count], r1_sem.at[g]).wait()

        def half_sum(r, b, cols):
            yt = xs[(r // 2) * nb + b].astype(F32).T.astype(BF16)
            return jnp.dot(yt, ct[r, b, :, cols], preferred_element_type=F32) * wrow[r, pl.ds(b, 1), :][:, cols]

        def comp(r, b, g):
            d2s[r, b] = half_sum(r, b, slice(tok, 2 * tok)).astype(BF16)
            d2_start(r, b, g)

        def mine(r, b):
            return half_sum(r, b, slice(0, tok))

        cut = tok // 2

        def h_start(b):
            for cols, send, dev in ((slice(0, cut), by_x, to_x), (slice(cut, tok), by_y, to_y)):
                remote(d2s.at[3, b, :, cols], hr.at[b, :, cols], send, r0_sem.at[b], dev).start()

        def f_start(b):
            remote(d2s.at[1, b], f1r.at[b], by_x, r0_sem.at[nb + b], to_x).start()
            remote(d2s.at[2, b], f2r.at[b], by_y, r0_sem.at[nb + b], to_y).start()

        @pl.loop(0, 2)
        def _(b):
            comp(3, b, b)

        @pl.loop(0, nb)
        def _(b):
            t = mine(3, b)
            d2_wait(b, 1)
            d2s[3, b] = (t + d2r[3, b].astype(F32)).astype(BF16)
            h_start(b)

            @pl.when(b < nb - 2)
            def _():
                comp(3, b + 2, b + 2)

        @pl.loop(0, nb)
        def _(b):
            comp(1, b, nb + b)
            comp(2, b, nb + b)

        def hop(b):
            t1, t2 = mine(1, b), mine(2, b)
            d2_wait(nb + b, 2)
            t1 += d2r[1, b].astype(F32)
            t2 += d2r[2, b].astype(F32)
            blocks(hr.at[0], r0_sem.at[b]).wait()
            h = hr[b].astype(F32)
            d2s[1, b] = jnp.concatenate([t1[:, :cut], t1[:, cut:] + h[:, cut:]], axis=1).astype(BF16)
            d2s[2, b] = jnp.concatenate([t2[:, :cut] + h[:, :cut], t2[:, cut:]], axis=1).astype(BF16)
            f_start(b)

        @pl.loop(0, 2)
        def _(b):
            hop(b)

        @pl.loop(0, nb)
        def _(b):
            comp(0, b, 2 * nb)

        @pl.loop(0, nb)
        def _(b):
            stash[b] = mine(0, b)

        @pl.loop(2, nb)
        def _(b):
            hop(b)

        d2_wait(2 * nb, nb)

        @pl.loop(0, nb)
        def _(b):
            base = stash[b] + d2r[0, b].astype(F32)
            blocks(f1r.at[0:2], r0_sem.at[nb + b]).wait()
            pos = s * tok + lax.broadcasted_iota(jnp.int32, (1, tok), 1)
            y = (base + f1r[b].astype(F32) + f2r[b].astype(F32)) / rqs[3, 0, pl.ds(nb + b, 1), :tok]
            y = jnp.where(pos < len_ref[b], y, 0.0)
            out_ref[b] = y.T.astype(BF16)

        blocks(xg.at[0, 0:3], by_x).wait()
        blocks(xg.at[0, 0:3], by_y).wait()

    pl.run_scoped(
        phase_combine,
        pltpu.VMEM((4, nb, dm, tok), BF16),
        pltpu.VMEM((nb, dm, tok), F32),
    )


def solution(mesh):
    def local_layer(tok_blk, len_blk, slot_param, logit_scale, w_in, w_out):
        nb, tok, dm = tok_blk.shape
        n_slots = slot_param.shape[1]
        slots = n_slots // 8
        ff = w_in.shape[2]
        hbm = pl.BlockSpec(memory_space=pl.ANY)
        dma = pltpu.SemaphoreType.DMA
        return pl.pallas_call(
            layer_kernel,
            out_shape=pltpu.VMEM((nb, tok, dm), BF16),
            in_specs=[hbm] * 6,
            out_specs=pl.BlockSpec(memory_space=pltpu.VMEM),
            scratch_shapes=[
                pltpu.SMEM((1,), F32),
                pltpu.SMEM((nb,), jnp.int32),
                pltpu.VMEM((4, nb, 2, tok, dm), BF16),
                pltpu.VMEM((4, 2, nb, tok), F32),
                pltpu.VMEM((4, 4, 2 * nb, 2 * tok), F32),
                pltpu.VMEM((3, 4, 2 * nb, 2 * tok), F32),
                pltpu.VMEM((4, nb, 2 * tok), F32),
                pltpu.VMEM((4, nb, slots, 2 * tok), BF16),
                pltpu.VMEM((2 * nb, slots, dm), BF16),
                pltpu.VMEM((4, nb, dm, tok), BF16),
                pltpu.VMEM((nb, dm, tok), BF16),
                pltpu.VMEM((nb, dm, tok), BF16),
                pltpu.VMEM((nb, dm, tok), BF16),
                pltpu.VMEM((RING, dm, ff), BF16),
                pltpu.VMEM((RING, ff, dm), BF16),
                dma((4,)), dma((RING,)), dma((3,)), dma((2 * nb,)), dma((3 * nb,)), dma((2,)), dma((5,)), dma((1,)), dma((3,)), dma((2 * nb + 1,)),
            ],
            compiler_params=pltpu.CompilerParams(collective_id=0, has_side_effects=True, vmem_limit_bytes=66_250_000),
            name="soft_moe_layer",
        )(logit_scale.reshape(1), len_blk, tok_blk, slot_param, w_in, w_out)

    return jax.shard_map(local_layer, mesh=mesh, in_specs=(P("data", "seq", None), P("data"), P(None, None), P(), P("seq", None, None), P("seq", None, None)), out_specs=P("data", "seq", None), check_vma=False)
```

```python
import functools
import math

import jax
import jax.numpy as jnp
from jax import lax
from jax.experimental import pallas as pl
from jax.experimental.pallas import tpu as pltpu
from jax.sharding import PartitionSpec as P

EPSILON = 1e-6
TOP = 3.4028235e38
LOG2E = 1.0 / math.log(2.0)
F32 = jnp.float32
BF16 = jnp.bfloat16
RING = 14


def unit_rows(v32):
    return (v32 * lax.rsqrt(jnp.sum(v32 * v32, axis=1, keepdims=True) + EPSILON)).astype(BF16)


def expd(a, b):
    return jnp.exp2((a - b) * LOG2E)


def gelu_tanh(h):
    inner = h * (math.sqrt(2.0 / math.pi) + (math.sqrt(2.0 / math.pi) * 0.044715) * (h * h))
    half = 0.5 * h
    return half + half * jnp.tanh(inner)


def layer_kernel(
    scale_hbm, len_hbm, x_hbm, phi_hbm, w1_hbm, w2_hbm, out_ref,
    scale_ref, len_ref, xg, rm, rqs, rqr, wrow, ct, xs, d2r, hr, f1r, f2r, w1b, w2b,
    in_sem, w_sem, send_sem, r0_sem, r1_sem, rms_sem, rmr_sem, rqs_sem, rqr_sem, d2s_sem,
):
    nb, tok, dm = x_hbm.shape
    slots = xs.shape[1]
    n_slots = phi_hbm.shape[1]
    n_exp = slots // 16
    d = lax.axis_index("data")
    s = lax.axis_index("seq")
    xc, core = s // 2, s % 2
    to_p = {"data": d, "seq": 2 * xc + (1 - core)}
    to_x = {"data": d, "seq": 2 * (1 - xc) + core}
    to_y = {"data": 1 - d, "seq": s}

    def remote(src, dst, send, recv, dev):
        return pltpu.make_async_remote_copy(src_ref=src, dst_ref=dst, send_sem=send, recv_sem=recv, device_id=dev, device_id_type=pl.DeviceIdType.MESH)

    def weight_copies(e, slot):
        return (
            pltpu.make_async_copy(w1_hbm.at[n_exp * d + e], w1b.at[slot], w_sem.at[slot]),
            pltpu.make_async_copy(w2_hbm.at[n_exp * d + e], w2b.at[slot], w_sem.at[slot]),
        )

    barrier = pltpu.get_barrier_semaphore()
    for dev in (to_p, to_x, to_y):
        pl.semaphore_signal(barrier, inc=1, device_id=dev, device_id_type=pl.DeviceIdType.MESH)

    phi = ct.at[3, nb - 1, 0:dm]
    pnt = xs.at[2 * nb - 1]
    loads = [
        pltpu.make_async_copy(x_hbm, xg.at[0, :, 0], in_sem.at[0]),
        pltpu.make_async_copy(phi_hbm.at[:, pl.ds(pl.multiple_of(s * (n_slots // 4) + d * slots, slots), slots)], phi, in_sem.at[1]),
        pltpu.make_async_copy(len_hbm, len_ref, in_sem.at[2]),
        pltpu.make_async_copy(scale_hbm, scale_ref, in_sem.at[3]),
    ]
    for c in loads:
        c.start()

    by_x, by_y, by_p = send_sem.at[0], send_sem.at[1], send_sem.at[2]

    def blocks(ref, sem):
        return pltpu.make_async_copy(ref, ref, sem)

    def send_x(b):
        return remote(xg.at[0, b, 0], xg.at[1, b, 0], by_x, r0_sem.at[b], to_x)

    def send_y(b):
        return remote(xg.at[0, b, 0], xg.at[2, b, 0], by_y, r0_sem.at[b], to_y)

    def send_p(b):
        return remote(xg.at[0, b, 0], xg.at[0, b, 1], by_p, r1_sem.at[b], to_p)

    def fwd_across(r, b, part, send, dev):
        remote(xg.at[r, b, 0, part], xg.at[3, b, 0, part], send, r0_sem.at[nb + b], dev).start()

    def arrive_pair(b):
        blocks(xg.at[0, 0], r0_sem.at[b]).wait()
        for r in (1, 2):
            remote(xg.at[r, b, 0], xg.at[r, b, 1], by_p, r1_sem.at[nb + b], to_p).start()
        fwd_across(1, b, slice(0, tok // 2), by_y, to_y)
        fwd_across(2, b, slice(tok // 2, tok), by_x, to_x)

    def arrive_across(b):
        blocks(xg.at[0, 0, 0], r0_sem.at[nb + b]).wait()
        remote(xg.at[3, b, 0], xg.at[3, b, 1], by_p, r1_sem.at[2 * nb + b], to_p).start()

    rm_x = remote(rm.at[0, 0], rm.at[1, 0], rms_sem.at[0], rmr_sem.at[0], to_x)
    rm_y = remote(rm.at[0, 0], rm.at[2, 0], rms_sem.at[0], rmr_sem.at[0], to_y)
    rm_f = remote(rm.at[1, 0], rm.at[3, 0], rms_sem.at[0], rmr_sem.at[1], to_y)
    rm_p = [remote(rm.at[r, 0], rm.at[r, 1], rms_sem.at[1], rmr_sem.at[(2, 3, 3, 4)[r]], to_p) for r in range(4)]

    def phase_dispatch(acc, m_s, z_s):
        loads[2].wait()
        pos = s * tok + lax.broadcasted_iota(jnp.int32, (1, tok), 1)
        for b in range(nb):
            rm[0, 0, b:b + 1, :] = jnp.where(pos < len_ref[b], TOP, -TOP)
        loads[0].wait()
        pl.semaphore_wait(barrier, 3)
        rm_x.start()
        rm_y.start()
        rm_p[0].start()
        for b in range(nb):
            send_x(b).start()
            send_y(b).start()
        for b in range(nb):
            send_p(b).start()
        for e in range(RING):
            for c in weight_copies(e, e):
                c.start()
        loads[3].wait()
        g = scale_ref[0]
        loads[1].wait()
        v = phi[...].astype(F32)
        pnt[...] = (v * lax.rsqrt(jnp.sum(v * v, axis=0, keepdims=True) + EPSILON)).T.astype(BF16)
        blocks(rm.at[0], rmr_sem.at[0]).wait()
        for c in (rm_f, rm_p[1], rm_p[2]):
            c.start()

        def unit(r, b, first, last):
            q = (r // 2) * nb + b
            a = b
            xb = xg[r, b].reshape(2 * tok, dm)
            xn = unit_rows(xb.astype(F32))
            lt = lax.dot_general(pnt[...], xn, (((1,), (1,)), ((), ())), preferred_element_type=F32) * g
            lm = jnp.minimum(lt, jnp.concatenate([rm[r, k, pl.ds(b, 1), :] for k in range(2)], axis=1))
            mx = jnp.broadcast_to(jnp.max(lm, axis=1, keepdims=True), (slots, 128))
            if not first:
                m_old = m_s[a]
                mx = jnp.maximum(mx, m_old)
            e = expd(lm, jnp.concatenate([mx] * 4, axis=1))
            z = (e[:, 0:128] + e[:, 128:256]) + (e[:, 256:384] + e[:, 384:512])
            part = jnp.dot(e.astype(BF16), xb, preferred_element_type=F32)
            cmax = jnp.max(lt, axis=0, keepdims=True)
            c = expd(lt, cmax)
            rqs[0, r, pl.ds(b, 1), :] = cmax
            rqs[0, r, pl.ds(nb + b, 1), :] = jnp.sum(c, axis=0, keepdims=True)
            ct[r, b] = c.astype(BF16)
            if not first:
                corr = expd(m_old, mx)
                z = z + z_s[a] * corr
                part = part + acc[a] * jnp.concatenate([corr] * 3, axis=1)
            if last:
                inv = 1.0 / jnp.broadcast_to(jnp.sum(z, axis=1, keepdims=True), (slots, 128))
                xs[q] = (part * jnp.concatenate([inv] * 3, axis=1)).astype(BF16)
            else:
                m_s[a] = mx
                z_s[a] = z
                acc[a] = part

        blocks(rm.at[0, 0], rmr_sem.at[2]).wait()

        @pl.loop(0, nb)
        def _(b):
            blocks(xg.at[0, 0, 0], r1_sem.at[b]).wait()
            unit(0, b, True, False)

        arrive_pair(0)
        blocks(rm.at[0], rmr_sem.at[3]).wait()

        @pl.loop(0, nb)
        def _(j):
            blocks(xg.at[0, 0], r1_sem.at[nb + j]).wait()
            unit(1, j, False, True)

            @pl.when(j < nb - 1)
            def _():
                arrive_pair(j + 1)

            @pl.when(j == nb - 1)
            def _():
                blocks(rm.at[0, 0], rmr_sem.at[1]).wait()
                rm_p[3].start()
                arrive_across(0)

            unit(2, j, True, False)

        arrive_across(1)
        blocks(rm.at[0, 0], rmr_sem.at[4]).wait()

        @pl.loop(0, nb)
        def _(b):
            @pl.when(b == nb - 2)
            def _():
                arrive_across(nb - 2)
                arrive_across(nb - 1)

            blocks(xg.at[0, 0, 0], r1_sem.at[2 * nb + b]).wait()
            unit(3, b, False, True)

        blocks(xg.at[0, 0:3], by_x).wait()
        blocks(xg.at[0, 0:3], by_y).wait()
        blocks(xg.at[0:2], by_p).wait()
        blocks(rm.at[0:3, 0], rms_sem.at[0]).wait()
        blocks(rm.at[0:2], rms_sem.at[1]).wait()

    pl.run_scoped(
        phase_dispatch,
        pltpu.VMEM((nb, slots, dm), F32),
        pltpu.VMEM((nb, slots, 128), F32),
        pltpu.VMEM((nb, slots, 128), F32),
    )

    rq_copies = [remote(rqs.at[k], rqr.at[k], rqs_sem.at[0], rqr_sem.at[k], dev) for k, dev in enumerate((to_p, to_x, to_y))]

    def merge(k):
        rq_copies[k].wait()
        for r in range(4):
            if k == 0:
                theirs = jnp.concatenate([rqr[k, r][:, tok:], rqr[k, r][:, :tok]], axis=1)
            else:
                theirs = rqr[k, r ^ k]
            mine = rqs[k, r]
            top = jnp.maximum(mine[:nb], theirs[:nb])
            low = mine[nb:] * expd(mine[:nb], top) + theirs[nb:] * expd(theirs[:nb], top)
            rqs[k + 1, r, :nb] = top
            rqs[k + 1, r, nb:] = low
            if k == 2:
                wrow[r] = expd(rqs[0, r][:nb], top)
        if k < 2:
            rq_copies[k + 1].start()

    rq_copies[0].start()

    def ffn(es):
        for e in es:
            blocks(w1b.at[0:2], w_sem.at[e % RING]).wait()
        rows = [pl.ds(pl.multiple_of(e * 16, 16), 16) for e in es]
        xe = [xs[:, r, :].reshape(2 * nb * 16, dm) for r in rows]
        hs = [jnp.dot(x, w1b[e % RING], preferred_element_type=F32) for x, e in zip(xe, es)]
        ys = [jnp.dot(gelu_tanh(h).astype(BF16), w2b[e % RING], preferred_element_type=F32) for h, e in zip(hs, es)]
        for y, r in zip(ys, rows):
            xs[:, r, :] = y.astype(BF16).reshape(2 * nb, 16, dm)
        for e in es:
            @pl.when(e + RING < n_exp)
            def _():
                for c in weight_copies(e + RING, e % RING):
                    c.start()

    ffn([0, 1])

    @pl.loop(0, (n_exp - 8) // 4)
    def _(i):
        ffn([4 * i + 2 + k for k in range(4)])
        for k in range(3):
            @pl.when(i == 2 * k + 1)
            def _():
                merge(k)

    @pl.loop(0, 3)
    def _(i):
        ffn([n_exp - 6 + 2 * i, n_exp - 5 + 2 * i])

    def phase_combine(d2s, stash):
        def d2_start(r, b, g):
            remote(d2s.at[r, b], d2r.at[r, b], d2s_sem.at[g], r1_sem.at[g], to_p).start()

        def d2_wait(g, count):
            blocks(d2s.at[0, 0:count], d2s_sem.at[g]).wait()
            blocks(d2r.at[0, 0:count], r1_sem.at[g]).wait()

        def half_sum(r, b, cols):
            yt = xs[(r // 2) * nb + b].astype(F32).T.astype(BF16)
            return jnp.dot(yt, ct[r, b, :, cols], preferred_element_type=F32) * wrow[r, pl.ds(b, 1), :][:, cols]

        def comp(r, b, g):
            d2s[r, b] = half_sum(r, b, slice(tok, 2 * tok)).astype(BF16)
            d2_start(r, b, g)

        def mine(r, b):
            return half_sum(r, b, slice(0, tok))

        cut = tok // 2

        def h_start(b):
            for cols, send, dev in ((slice(0, cut), by_x, to_x), (slice(cut, tok), by_y, to_y)):
                remote(d2s.at[3, b, :, cols], hr.at[b, :, cols], send, r0_sem.at[b], dev).start()

        def f_start(b):
            remote(d2s.at[1, b], f1r.at[b], by_x, r0_sem.at[nb + b], to_x).start()
            remote(d2s.at[2, b], f2r.at[b], by_y, r0_sem.at[nb + b], to_y).start()

        @pl.loop(0, 2)
        def _(b):
            comp(3, b, b)

        @pl.loop(0, nb)
        def _(b):
            t = mine(3, b)
            d2_wait(b, 1)
            d2s[3, b] = (t + d2r[3, b].astype(F32)).astype(BF16)
            h_start(b)

            @pl.when(b < nb - 2)
            def _():
                comp(3, b + 2, b + 2)

        @pl.loop(0, nb)
        def _(b):
            comp(1, b, nb + b)
            comp(2, b, nb + b)

        def hop(b):
            t1, t2 = mine(1, b), mine(2, b)
            d2_wait(nb + b, 2)
            t1 += d2r[1, b].astype(F32)
            t2 += d2r[2, b].astype(F32)
            blocks(hr.at[0], r0_sem.at[b]).wait()
            h = hr[b].astype(F32)
            d2s[1, b] = jnp.concatenate([t1[:, :cut], t1[:, cut:] + h[:, cut:]], axis=1).astype(BF16)
            d2s[2, b] = jnp.concatenate([t2[:, :cut] + h[:, :cut], t2[:, cut:]], axis=1).astype(BF16)
            f_start(b)

        @pl.loop(0, 2)
        def _(b):
            hop(b)

        @pl.loop(0, nb)
        def _(b):
            comp(0, b, 2 * nb)

        @pl.loop(0, nb)
        def _(b):
            stash[b] = mine(0, b)

        @pl.loop(2, nb)
        def _(b):
            hop(b)

        d2_wait(2 * nb, nb)

        @pl.loop(0, nb)
        def _(b):
            base = stash[b] + d2r[0, b].astype(F32)
            blocks(f1r.at[0:2], r0_sem.at[nb + b]).wait()
            pos = s * tok + lax.broadcasted_iota(jnp.int32, (1, tok), 1)
            y = (base + f1r[b].astype(F32) + f2r[b].astype(F32)) / rqs[3, 0, pl.ds(nb + b, 1), :tok]
            y = jnp.where(pos < len_ref[b], y, 0.0)
            out_ref[b] = y.T.astype(BF16)

        blocks(xg.at[0, 0:3], by_x).wait()
        blocks(xg.at[0, 0:3], by_y).wait()

    pl.run_scoped(
        phase_combine,
        pltpu.VMEM((4, nb, dm, tok), BF16),
        pltpu.VMEM((nb, dm, tok), F32),
    )


def solution(mesh):
    def local_layer(tok_blk, len_blk, slot_param, logit_scale, w_in, w_out):
        nb, tok, dm = tok_blk.shape
        n_slots = slot_param.shape[1]
        slots = n_slots // 8
        ff = w_in.shape[2]
        hbm = pl.BlockSpec(memory_space=pl.ANY)
        dma = pltpu.SemaphoreType.DMA
        return pl.pallas_call(
            layer_kernel,
            out_shape=pltpu.VMEM((nb, tok, dm), BF16),
            in_specs=[hbm] * 6,
            out_specs=pl.BlockSpec(memory_space=pltpu.VMEM),
            scratch_shapes=[
                pltpu.SMEM((1,), F32),
                pltpu.SMEM((nb,), jnp.int32),
                pltpu.VMEM((4, nb, 2, tok, dm), BF16),
                pltpu.VMEM((4, 2, nb, tok), F32),
                pltpu.VMEM((4, 4, 2 * nb, 2 * tok), F32),
                pltpu.VMEM((3, 4, 2 * nb, 2 * tok), F32),
                pltpu.VMEM((4, nb, 2 * tok), F32),
                pltpu.VMEM((4, nb, slots, 2 * tok), BF16),
                pltpu.VMEM((2 * nb, slots, dm), BF16),
                pltpu.VMEM((4, nb, dm, tok), BF16),
                pltpu.VMEM((nb, dm, tok), BF16),
                pltpu.VMEM((nb, dm, tok), BF16),
                pltpu.VMEM((nb, dm, tok), BF16),
                pltpu.VMEM((RING, dm, ff), BF16),
                pltpu.VMEM((RING, ff, dm), BF16),
                dma((4,)), dma((RING,)), dma((3,)), dma((2 * nb,)), dma((3 * nb,)), dma((2,)), dma((5,)), dma((1,)), dma((3,)), dma((2 * nb + 1,)),
            ],
            compiler_params=pltpu.CompilerParams(collective_id=0, has_side_effects=True, vmem_limit_bytes=66_250_000),
            name="soft_moe_layer",
        )(logit_scale.reshape(1), len_blk, tok_blk, slot_param, w_in, w_out)

    return jax.shard_map(local_layer, mesh=mesh, in_specs=(P("data", "seq", None), P("data"), P(None, None), P(), P("seq", None, None), P("seq", None, None)), out_specs=P("data", "seq", None), check_vma=False)
```

```python
import functools
import math

import jax
import jax.numpy as jnp
from jax import lax
from jax.experimental import pallas as pl
from jax.experimental.pallas import tpu as pltpu
from jax.sharding import PartitionSpec as P

EPSILON = 1e-6
TOP = 3.4028235e38
LOG2E = 1.0 / math.log(2.0)
F32 = jnp.float32
BF16 = jnp.bfloat16
RING = 14


def unit_rows(v32):
    return (v32 * lax.rsqrt(jnp.sum(v32 * v32, axis=1, keepdims=True) + EPSILON)).astype(BF16)


def expd(a, b):
    return jnp.exp2((a - b) * LOG2E)


def gelu_tanh(h):
    inner = h * (math.sqrt(2.0 / math.pi) + (math.sqrt(2.0 / math.pi) * 0.044715) * (h * h))
    half = 0.5 * h
    return half + half * jnp.tanh(inner)


def layer_kernel(
    scale_hbm, len_hbm, x_hbm, phi_hbm, w1_hbm, w2_hbm, out_ref,
    scale_ref, len_ref, xg, rm, rqs, rqr, wrow, ct, xs, d2r, hr, f1r, f2r, w1b, w2b,
    in_sem, w_sem, send_sem, r0_sem, r1_sem, rms_sem, rmr_sem, rqs_sem, rqr_sem, d2s_sem,
):
    nb, tok, dm = x_hbm.shape
    slots = xs.shape[1]
    n_slots = phi_hbm.shape[1]
    n_exp = slots // 16
    d = lax.axis_index("data")
    s = lax.axis_index("seq")
    xc, core = s // 2, s % 2
    to_p = {"data": d, "seq": 2 * xc + (1 - core)}
    to_x = {"data": d, "seq": 2 * (1 - xc) + core}
    to_y = {"data": 1 - d, "seq": s}

    def remote(src, dst, send, recv, dev):
        return pltpu.make_async_remote_copy(src_ref=src, dst_ref=dst, send_sem=send, recv_sem=recv, device_id=dev, device_id_type=pl.DeviceIdType.MESH)

    def weight_copies(e, slot):
        return (
            pltpu.make_async_copy(w1_hbm.at[n_exp * d + e], w1b.at[slot], w_sem.at[slot]),
            pltpu.make_async_copy(w2_hbm.at[n_exp * d + e], w2b.at[slot], w_sem.at[slot]),
        )

    barrier = pltpu.get_barrier_semaphore()
    for dev in (to_p, to_x, to_y):
        pl.semaphore_signal(barrier, inc=1, device_id=dev, device_id_type=pl.DeviceIdType.MESH)

    phi = ct.at[3, nb - 1, 0:dm]
    pnt = xs.at[2 * nb - 1]
    loads = [
        pltpu.make_async_copy(x_hbm, xg.at[0, :, 0], in_sem.at[0]),
        pltpu.make_async_copy(phi_hbm.at[:, pl.ds(pl.multiple_of(s * (n_slots // 4) + d * slots, slots), slots)], phi, in_sem.at[1]),
        pltpu.make_async_copy(len_hbm, len_ref, in_sem.at[2]),
        pltpu.make_async_copy(scale_hbm, scale_ref, in_sem.at[3]),
    ]
    for c in loads:
        c.start()

    by_x, by_y, by_p = send_sem.at[0], send_sem.at[1], send_sem.at[2]

    def blocks(ref, sem):
        return pltpu.make_async_copy(ref, ref, sem)

    def send_x(b):
        return remote(xg.at[0, b, 0], xg.at[1, b, 0], by_x, r0_sem.at[b], to_x)

    def send_y(b):
        return remote(xg.at[0, b, 0], xg.at[2, b, 0], by_y, r0_sem.at[b], to_y)

    def send_p(b):
        return remote(xg.at[0, b, 0], xg.at[0, b, 1], by_p, r1_sem.at[b], to_p)

    def fwd_across(r, b, part, send, dev):
        remote(xg.at[r, b, 0, part], xg.at[3, b, 0, part], send, r0_sem.at[nb + b], dev).start()

    def arrive_pair(b):
        blocks(xg.at[0, 0], r0_sem.at[b]).wait()
        for r in (1, 2):
            remote(xg.at[r, b, 0], xg.at[r, b, 1], by_p, r1_sem.at[nb + b], to_p).start()
        fwd_across(1, b, slice(0, tok // 2), by_y, to_y)
        fwd_across(2, b, slice(tok // 2, tok), by_x, to_x)

    def arrive_across(b):
        blocks(xg.at[0, 0, 0], r0_sem.at[nb + b]).wait()
        remote(xg.at[3, b, 0], xg.at[3, b, 1], by_p, r1_sem.at[2 * nb + b], to_p).start()

    rm_x = remote(rm.at[0, 0], rm.at[1, 0], rms_sem.at[0], rmr_sem.at[0], to_x)
    rm_y = remote(rm.at[0, 0], rm.at[2, 0], rms_sem.at[0], rmr_sem.at[0], to_y)
    rm_f = remote(rm.at[1, 0], rm.at[3, 0], rms_sem.at[0], rmr_sem.at[1], to_y)
    rm_p = [remote(rm.at[r, 0], rm.at[r, 1], rms_sem.at[1], rmr_sem.at[(2, 3, 3, 4)[r]], to_p) for r in range(4)]

    def phase_dispatch(acc, m_s, z_s):
        loads[2].wait()
        pos = s * tok + lax.broadcasted_iota(jnp.int32, (1, tok), 1)
        for b in range(nb):
            rm[0, 0, b:b + 1, :] = jnp.where(pos < len_ref[b], TOP, -TOP)
        loads[0].wait()
        pl.semaphore_wait(barrier, 3)
        rm_x.start()
        rm_y.start()
        rm_p[0].start()
        for b in range(nb):
            send_x(b).start()
            send_y(b).start()
        for b in range(nb):
            send_p(b).start()
        for e in range(RING):
            for c in weight_copies(e, e):
                c.start()
        loads[3].wait()
        g = scale_ref[0]
        loads[1].wait()
        v = phi[...].astype(F32)
        pnt[...] = (v * lax.rsqrt(jnp.sum(v * v, axis=0, keepdims=True) + EPSILON)).T.astype(BF16)
        blocks(rm.at[0], rmr_sem.at[0]).wait()
        for c in (rm_f, rm_p[1], rm_p[2]):
            c.start()

        def unit(r, b, first, last):
            q = (r // 2) * nb + b
            a = b
            xb = xg[r, b].reshape(2 * tok, dm)
            xn = unit_rows(xb.astype(F32))
            lt = lax.dot_general(pnt[...], xn, (((1,), (1,)), ((), ())), preferred_element_type=F32) * g
            lm = jnp.minimum(lt, jnp.concatenate([rm[r, k, pl.ds(b, 1), :] for k in range(2)], axis=1))
            mx = jnp.broadcast_to(jnp.max(lm, axis=1, keepdims=True), (slots, 128))
            if not first:
                m_old = m_s[a]
                mx = jnp.maximum(mx, m_old)
            e = expd(lm, jnp.concatenate([mx] * 4, axis=1))
            z = (e[:, 0:128] + e[:, 128:256]) + (e[:, 256:384] + e[:, 384:512])
            part = jnp.dot(e.astype(BF16), xb, preferred_element_type=F32)
            cmax = jnp.max(lt, axis=0, keepdims=True)
            c = expd(lt, cmax)
            rqs[0, r, pl.ds(b, 1), :] = cmax
            rqs[0, r, pl.ds(nb + b, 1), :] = jnp.sum(c, axis=0, keepdims=True)
            ct[r, b] = c.astype(BF16)
            if not first:
                corr = expd(m_old, mx)
                z = z + z_s[a] * corr
                part = part + acc[a] * jnp.concatenate([corr] * 3, axis=1)
            if last:
                inv = 1.0 / jnp.broadcast_to(jnp.sum(z, axis=1, keepdims=True), (slots, 128))
                xs[q] = (part * jnp.concatenate([inv] * 3, axis=1)).astype(BF16)
            else:
                m_s[a] = mx
                z_s[a] = z
                acc[a] = part

        blocks(rm.at[0, 0], rmr_sem.at[2]).wait()

        @pl.loop(0, nb)
        def _(b):
            blocks(xg.at[0, 0, 0], r1_sem.at[b]).wait()
            unit(0, b, True, False)

        arrive_pair(0)
        blocks(rm.at[0], rmr_sem.at[3]).wait()

        @pl.loop(0, nb)
        def _(j):
            blocks(xg.at[0, 0], r1_sem.at[nb + j]).wait()
            unit(1, j, False, True)

            @pl.when(j < nb - 1)
            def _():
                arrive_pair(j + 1)

            @pl.when(j == nb - 1)
            def _():
                blocks(rm.at[0, 0], rmr_sem.at[1]).wait()
                rm_p[3].start()
                arrive_across(0)

            unit(2, j, True, False)

        arrive_across(1)
        blocks(rm.at[0, 0], rmr_sem.at[4]).wait()

        @pl.loop(0, nb)
        def _(b):
            @pl.when(b == nb - 2)
            def _():
                arrive_across(nb - 2)
                arrive_across(nb - 1)

            blocks(xg.at[0, 0, 0], r1_sem.at[2 * nb + b]).wait()
            unit(3, b, False, True)

        blocks(xg.at[0, 0:3], by_x).wait()
        blocks(xg.at[0, 0:3], by_y).wait()
        blocks(xg.at[0:2], by_p).wait()
        blocks(rm.at[0:3, 0], rms_sem.at[0]).wait()
        blocks(rm.at[0:2], rms_sem.at[1]).wait()

    pl.run_scoped(
        phase_dispatch,
        pltpu.VMEM((nb, slots, dm), F32),
        pltpu.VMEM((nb, slots, 128), F32),
        pltpu.VMEM((nb, slots, 128), F32),
    )

    rq_copies = [remote(rqs.at[k], rqr.at[k], rqs_sem.at[0], rqr_sem.at[k], dev) for k, dev in enumerate((to_p, to_x, to_y))]

    def merge(k):
        rq_copies[k].wait()
        for r in range(4):
            if k == 0:
                theirs = jnp.concatenate([rqr[k, r][:, tok:], rqr[k, r][:, :tok]], axis=1)
            else:
                theirs = rqr[k, r ^ k]
            mine = rqs[k, r]
            top = jnp.maximum(mine[:nb], theirs[:nb])
            low = mine[nb:] * expd(mine[:nb], top) + theirs[nb:] * expd(theirs[:nb], top)
            rqs[k + 1, r, :nb] = top
            rqs[k + 1, r, nb:] = low
            if k == 2:
                wrow[r] = expd(rqs[0, r][:nb], top)
        if k < 2:
            rq_copies[k + 1].start()

    rq_copies[0].start()

    def ffn(es):
        for e in es:
            blocks(w1b.at[0:2], w_sem.at[e % RING]).wait()
        rows = [pl.ds(pl.multiple_of(e * 16, 16), 16) for e in es]
        xe = [xs[:, r, :].reshape(2 * nb * 16, dm) for r in rows]
        hs = [jnp.dot(x, w1b[e % RING], preferred_element_type=F32) for x, e in zip(xe, es)]
        ys = [jnp.dot(gelu_tanh(h).astype(BF16), w2b[e % RING], preferred_element_type=F32) for h, e in zip(hs, es)]
        for y, r in zip(ys, rows):
            xs[:, r, :] = y.astype(BF16).reshape(2 * nb, 16, dm)
        for e in es:
            @pl.when(e + RING < n_exp)
            def _():
                for c in weight_copies(e + RING, e % RING):
                    c.start()

    ffn([0, 1])

    @pl.loop(0, (n_exp - 8) // 4)
    def _(i):
        ffn([4 * i + 2 + k for k in range(4)])
        for k in range(3):
            @pl.when(i == 2 * k + 1)
            def _():
                merge(k)

    @pl.loop(0, 3)
    def _(i):
        ffn([n_exp - 6 + 2 * i, n_exp - 5 + 2 * i])

    def phase_combine(d2s, stash):
        def d2_start(r, b, g):
            remote(d2s.at[r, b], d2r.at[r, b], d2s_sem.at[g], r1_sem.at[g], to_p).start()

        def d2_wait(g, count):
            blocks(d2s.at[0, 0:count], d2s_sem.at[g]).wait()
            blocks(d2r.at[0, 0:count], r1_sem.at[g]).wait()

        def half_sum(r, b, cols):
            yt = xs[(r // 2) * nb + b].T
            return jnp.dot(yt, ct[r, b, :, cols], preferred_element_type=F32) * wrow[r, pl.ds(b, 1), :][:, cols]

        def comp(r, b, g):
            d2s[r, b] = half_sum(r, b, slice(tok, 2 * tok)).astype(BF16)
            d2_start(r, b, g)

        def mine(r, b):
            return half_sum(r, b, slice(0, tok))

        cut = tok // 2

        def h_start(b):
            for cols, send, dev in ((slice(0, cut), by_x, to_x), (slice(cut, tok), by_y, to_y)):
                remote(d2s.at[3, b, :, cols], hr.at[b, :, cols], send, r0_sem.at[b], dev).start()

        def f_start(b):
            remote(d2s.at[1, b], f1r.at[b], by_x, r0_sem.at[nb + b], to_x).start()
            remote(d2s.at[2, b], f2r.at[b], by_y, r0_sem.at[nb + b], to_y).start()

        @pl.loop(0, 2)
        def _(b):
            comp(3, b, b)

        @pl.loop(0, nb)
        def _(b):
            t = mine(3, b)
            d2_wait(b, 1)
            d2s[3, b] = (t + d2r[3, b].astype(F32)).astype(BF16)
            h_start(b)

            @pl.when(b < nb - 2)
            def _():
                comp(3, b + 2, b + 2)

        @pl.loop(0, nb)
        def _(b):
            comp(1, b, nb + b)
            comp(2, b, nb + b)

        def hop(b):
            t1, t2 = mine(1, b), mine(2, b)
            d2_wait(nb + b, 2)
            t1 += d2r[1, b].astype(F32)
            t2 += d2r[2, b].astype(F32)
            blocks(hr.at[0], r0_sem.at[b]).wait()
            h = hr[b].astype(F32)
            d2s[1, b] = jnp.concatenate([t1[:, :cut], t1[:, cut:] + h[:, cut:]], axis=1).astype(BF16)
            d2s[2, b] = jnp.concatenate([t2[:, :cut] + h[:, :cut], t2[:, cut:]], axis=1).astype(BF16)
            f_start(b)

        @pl.loop(0, 2)
        def _(b):
            hop(b)

        @pl.loop(0, nb)
        def _(b):
            comp(0, b, 2 * nb)

        @pl.loop(0, nb)
        def _(b):
            stash[b] = mine(0, b)

        @pl.loop(2, nb)
        def _(b):
            hop(b)

        d2_wait(2 * nb, nb)

        @pl.loop(0, nb)
        def _(b):
            base = stash[b] + d2r[0, b].astype(F32)
            blocks(f1r.at[0:2], r0_sem.at[nb + b]).wait()
            pos = s * tok + lax.broadcasted_iota(jnp.int32, (1, tok), 1)
            y = (base + f1r[b].astype(F32) + f2r[b].astype(F32)) * (1.0 / rqs[3, 0, pl.ds(nb + b, 1), :tok])
            y = jnp.where(pos < len_ref[b], y, 0.0)
            out_ref[b] = y.astype(BF16).T

        blocks(xg.at[0, 0:3], by_x).wait()
        blocks(xg.at[0, 0:3], by_y).wait()

    pl.run_scoped(
        phase_combine,
        pltpu.VMEM((4, nb, dm, tok), BF16),
        pltpu.VMEM((nb, dm, tok), F32),
    )


def solution(mesh):
    def local_layer(tok_blk, len_blk, slot_param, logit_scale, w_in, w_out):
        nb, tok, dm = tok_blk.shape
        n_slots = slot_param.shape[1]
        slots = n_slots // 8
        ff = w_in.shape[2]
        hbm = pl.BlockSpec(memory_space=pl.ANY)
        dma = pltpu.SemaphoreType.DMA
        return pl.pallas_call(
            layer_kernel,
            out_shape=pltpu.VMEM((nb, tok, dm), BF16),
            in_specs=[hbm] * 6,
            out_specs=pl.BlockSpec(memory_space=pltpu.VMEM),
            scratch_shapes=[
                pltpu.SMEM((1,), F32),
                pltpu.SMEM((nb,), jnp.int32),
                pltpu.VMEM((4, nb, 2, tok, dm), BF16),
                pltpu.VMEM((4, 2, nb, tok), F32),
                pltpu.VMEM((4, 4, 2 * nb, 2 * tok), F32),
                pltpu.VMEM((3, 4, 2 * nb, 2 * tok), F32),
                pltpu.VMEM((4, nb, 2 * tok), F32),
                pltpu.VMEM((4, nb, slots, 2 * tok), BF16),
                pltpu.VMEM((2 * nb, slots, dm), BF16),
                pltpu.VMEM((4, nb, dm, tok), BF16),
                pltpu.VMEM((nb, dm, tok), BF16),
                pltpu.VMEM((nb, dm, tok), BF16),
                pltpu.VMEM((nb, dm, tok), BF16),
                pltpu.VMEM((RING, dm, ff), BF16),
                pltpu.VMEM((RING, ff, dm), BF16),
                dma((4,)), dma((RING,)), dma((3,)), dma((2 * nb,)), dma((3 * nb,)), dma((2,)), dma((5,)), dma((1,)), dma((3,)), dma((2 * nb + 1,)),
            ],
            compiler_params=pltpu.CompilerParams(collective_id=0, has_side_effects=True, vmem_limit_bytes=66_250_000),
            name="soft_moe_layer",
        )(logit_scale.reshape(1), len_blk, tok_blk, slot_param, w_in, w_out)

    return jax.shard_map(local_layer, mesh=mesh, in_specs=(P("data", "seq", None), P("data"), P(None, None), P(), P("seq", None, None), P("seq", None, None)), out_specs=P("data", "seq", None), check_vma=False)
```
